128 devices in a mesh: cls: 128 (over y, x, z, core).
Axes of the slice: x: 4, y: 4, z: 4, core: 2. Of those that a mesh axis runs over, the one named last changes fastest.
Arguments:
- features: bfloat16 [2048, 12544], P('cls'), may hold values from -6 to 6
- fc_weight: bfloat16 [12544, 512], replicated, may hold values from -0.0546875 to 0.0546875
- centers: bfloat16 [524288, 512], P('cls'), may hold values from -6 to 6
- labels: int32 [2048], replicated, may hold values from 0 to 524287
Outputs:
- loss: float32 [2048], P('cls')
- grad_centers: bfloat16 [524288, 512], P('cls')
- grad_fc: float32 [12544, 512], P('cls')
The draws below stay inside these ranges and needn't reach their ends.
All inputs are finite; a program needn't handle non-finite values.
Results may differ from the reference program's by a relative error of at most 0.0078.
Values may be sent and summed in bfloat16 or wider, within the bound.
No kernel may reach another device: no remote copies, remote signals or barrier semaphores. Data moves between devices by JAX's collectives and lax.ppermute only.
A program may use at most 128 MiB of HBM per device.

```python
import math
import jax
import jax.numpy as jnp
from jax import lax

D = 512
F = 12544
C_DEV = 4096
B = 2048
C = 524288
N_CLS = 128


def place_ends(entries, own_key, least, top_value):
    longest = entries.shape.index(max(entries.shape))
    spots = []
    for shift in (0, 1):
        where = [jax.random.randint(jax.random.fold_in(own_key, axis), (), 0, length) for axis, length in enumerate(entries.shape)]
        where[longest] = (where[longest] + shift) % entries.shape[longest]
        spots.append(tuple(where))
    return entries.at[spots[0]].set(least).at[spots[1]].set(top_value)


def levels(key, shape, cuts, smallest, largest):
    level, own = 1.0, jax.random.fold_in(key, 6)
    for position, blocks in cuts:
        steps = jnp.exp(jax.random.uniform(jax.random.fold_in(own, position), (blocks,), jnp.float32, smallest / len(cuts), largest / len(cuts)))
        level = level * jnp.repeat(steps, shape[position] // blocks).reshape([-1 if axis == position else 1 for axis in range(len(shape))])
    return level


def gaussian(key, shape, deviation, reach, split=(), held_as=jnp.bfloat16):
    result = deviation * jax.random.normal(key, shape, jnp.float32)
    if split:
        result = result * levels(key, shape, split, -0.22, 0.18)
    return jnp.clip(result, -reach, reach).astype(held_as)


def setup_inputs(seed: int = 0) -> dict:
    key_list = jax.random.split(jax.random.key(seed), 5)
    return {
        "features": gaussian(key_list[0], (B, F), 1.0, 6.0, ((0, 128),)),
        "fc_weight": gaussian(key_list[1], (F, D), F ** -0.5, 0.0546875),
        "centers": gaussian(key_list[2], (C, D), 1.0, 6.0, ((0, 128),)),
        "labels": place_ends(jax.random.randint(key_list[3], (B,), 0, C), jax.random.fold_in(key_list[3], 1), 0, C - 1).astype(jnp.int32),
    }


logit_scale = 64.0
cos_margin = math.cos(0.5)
sin_margin = math.sin(0.5)
epsilon = 1e-06

def inverse_norm(values):
    return lax.rsqrt(lax.optimization_barrier(jnp.sum(values * values, axis=1, keepdims=True)) + epsilon)

def margin_logits(emb_low, center_low, labels, offset):
    cosines = jnp.dot(emb_low, center_low.T, preferred_element_type=jnp.float32)
    local_ids = labels - offset
    is_target = local_ids[:, None] == lax.broadcasted_iota(jnp.int32, (1, center_low.shape[0]), 1)
    target_cos = lax.optimization_barrier(jnp.sum(jnp.where(is_target, cosines, 0.0), axis=1))
    target_sine = jnp.sqrt(1.0 - target_cos * target_cos)
    margined = target_cos * cos_margin - target_sine * sin_margin
    logits = logit_scale * jnp.where(is_target, margined[:, None], cosines)
    slope = cos_margin + sin_margin * target_cos / target_sine
    return (logits, is_target, slope)

def center_parts(block):
    center_float = block.astype(jnp.float32)
    inv_center = inverse_norm(center_float)
    center_dir = center_float * inv_center
    return (inv_center, center_dir, center_dir.astype(jnp.bfloat16))

def reference(features, fc_weight, centers, labels):
    batch = labels.shape[0]
    embedded = jnp.dot(features, fc_weight, preferred_element_type=jnp.float32).astype(jnp.bfloat16)
    emb_float = embedded.astype(jnp.float32)
    inv_emb = inverse_norm(emb_float)
    emb_dir = emb_float * inv_emb
    emb_low = emb_dir.astype(jnp.bfloat16)
    blocks = centers.reshape(N_CLS, C_DEV, D)
    shard_ids = jnp.arange(N_CLS, dtype=jnp.int32)

    def stats_step(carry, item):
        shard, block = item
        unused_inv, unused_dir, center_low = center_parts(block)
        logits, is_target, unused_slope = margin_logits(emb_low, center_low, labels, shard * C_DEV)
        running_sum, target_sum = carry
        running_sum = running_sum + lax.optimization_barrier(jnp.sum(jnp.exp(logits - logit_scale), axis=1))
        target_sum = target_sum + lax.optimization_barrier(jnp.sum(jnp.where(is_target, logits, 0.0), axis=1))
        return ((running_sum, target_sum), None)
    start_stats = (jnp.zeros((batch,), jnp.float32), jnp.zeros((batch,), jnp.float32))
    (row_sum, target_sum), unused_out = lax.scan(stats_step, start_stats, (shard_ids, blocks))
    log_total = logit_scale + jnp.log(row_sum)
    loss = log_total - target_sum

    def grad_step(grad_dir, item):
        shard, block = item
        inv_center, center_dir, center_low = center_parts(block)
        logits, is_target, slope = margin_logits(emb_low, center_low, labels, shard * C_DEV)
        probs = jnp.exp(logits - log_total[:, None])
        grad_cos = (logit_scale * (probs - is_target.astype(jnp.float32)) * jnp.where(is_target, slope[:, None], 1.0)).astype(jnp.bfloat16)
        grad_unit = jnp.dot(grad_cos.T, emb_low, preferred_element_type=jnp.float32)
        grad_center = ((grad_unit - center_dir * lax.optimization_barrier(jnp.sum(grad_unit * center_dir, axis=1, keepdims=True))) * inv_center).astype(jnp.bfloat16)
        grad_dir = grad_dir + jnp.dot(grad_cos, center_low, preferred_element_type=jnp.float32)
        return (grad_dir, grad_center)
    grad_dir, grad_blocks = lax.scan(grad_step, jnp.zeros((batch, D), jnp.float32), (shard_ids, blocks))
    grad_centers = grad_blocks.reshape(N_CLS * C_DEV, D)
    grad_emb = ((grad_dir - emb_dir * lax.optimization_barrier(jnp.sum(grad_dir * emb_dir, axis=1, keepdims=True))) * inv_emb).astype(jnp.bfloat16)
    grad_fc = jnp.dot(features.T, grad_emb, preferred_element_type=jnp.float32)
    return (loss, grad_centers, grad_fc)
```

```python
import functools
import math

import jax
import jax.numpy as jnp
from jax import lax
from jax.experimental import pallas as pl
from jax.experimental.pallas import tpu as pltpu
from jax.sharding import Mesh
from jax.sharding import PartitionSpec as P

CLS = ("cls_0", "cls_1", "cls_2", "cls_3")
CHIP = ("cls_0", "cls_1", "cls_2")
CORE = "cls_3"

logit_scale = 64.0
cos_margin = math.cos(0.5)
sin_margin = math.sin(0.5)
epsilon = 1e-06

f32 = jnp.float32
bf16 = jnp.bfloat16
MIB = 1024 * 1024


def swapped(x):
    return lax.ppermute(x, CORE, [(0, 1), (1, 0)])


def to_chips(x):
    return lax.all_to_all(x, CHIP, split_axis=0, concat_axis=0, tiled=True)


def from_chips(x):
    copies = jnp.broadcast_to(x, (lax.axis_size(CHIP), *x.shape))
    return lax.all_to_all(copies, CHIP, split_axis=0, concat_axis=0, tiled=True)


def inverse_norm(values, axis):
    return lax.rsqrt(jnp.sum(values * values, axis=axis, keepdims=True) + epsilon)


def margin(target_cos):
    target_sine = jnp.sqrt(1.0 - target_cos * target_cos)
    margined = target_cos * cos_margin - target_sine * sin_margin
    slope = cos_margin + sin_margin * target_cos / target_sine
    return margined, slope


def centers_kernel(base, steps, ids_ref, c_ref, *refs):
    if base:
        refs = refs[2:]
    low_ref, turned_ref, found_ref = refs[:3]
    i = pl.program_id(0)
    rows = c_ref.shape[0]
    block = c_ref[...].astype(f32)
    low = (block * inverse_norm(block, 1)).astype(bf16)
    low_ref[...] = low
    turned = low.T
    turned_ref[...] = turned
    ids = ids_ref[...] - (base + i) * rows
    hit = lax.broadcasted_iota(jnp.int32, (rows, ids.shape[1]), 0) == ids
    rows_here = jnp.dot(turned, jnp.where(hit, 1.0, 0.0).astype(bf16), preferred_element_type=f32)

    @pl.when(i == 0)
    def _():
        found_ref[...] = rows_here

    @pl.when(i > 0)
    def _():
        found_ref[...] += rows_here


def prepared_centers(centers, ids, old, half, halves, rows=512):
    count, depth = centers.shape
    steps = count // rows
    base = half * steps
    samples = ids.shape[1]
    whole = halves * count
    old = () if old is None else old
    return pl.pallas_call(
        functools.partial(centers_kernel, base, steps),
        grid=(steps,),
        in_specs=[
            pl.BlockSpec((1, samples), lambda i: (0, 0)),
            pl.BlockSpec((rows, depth), lambda i: (i, 0)),
        ]
        + [pl.BlockSpec(memory_space=pl.ANY)] * len(old),
        out_specs=[
            pl.BlockSpec((rows, depth), lambda i: (base + i, 0)),
            pl.BlockSpec((depth, rows), lambda i: (0, base + i)),
            pl.BlockSpec((depth, samples), lambda i: (0, 0)),
        ],
        out_shape=[
            jax.ShapeDtypeStruct((whole, depth), bf16),
            jax.ShapeDtypeStruct((depth, whole), bf16),
            jax.ShapeDtypeStruct((depth, samples), f32),
        ],
        input_output_aliases={2: 0, 3: 1} if old else {},
        compiler_params=pltpu.CompilerParams(vmem_limit_bytes=24 * MIB),
        cost_estimate=pl.CostEstimate(
            flops=2 * count * depth * samples, bytes_accessed=6 * count * depth, transcendentals=0
        ),
        name=f"centers_{half}",
    )(ids, centers, *old)


def logits_kernel(sub, x_ref, ids_ref, found_ref, low_ref, turned_ref, exp_ref, sums_ref, pull_ref, stat_ref,
                  emb_ref, turned_emb, total, row_sum):
    i = pl.program_id(0)
    rows = low_ref.shape[0]
    samples = x_ref.shape[0]

    @pl.when(i == 0)
    def _():
        x = x_ref[...].astype(f32)
        emb = (x * inverse_norm(x, 1)).astype(bf16)
        emb_ref[...] = emb
        turned_emb[...] = (emb * logit_scale).astype(bf16).T
        total[...] = jnp.zeros_like(total)
        row_sum[...] = jnp.zeros_like(row_sum)

    low = low_ref[...]
    turned = turned_ref[...]
    here = lax.broadcasted_iota(jnp.int32, (rows, sub), 0)
    parts = samples // sub
    logits = jnp.dot(low, turned_emb[:, :sub], preferred_element_type=f32)
    for s in range(parts):
        span = slice(s * sub, (s + 1) * sub)
        if s + 1 < parts:
            later = jnp.dot(low, turned_emb[:, (s + 1) * sub : (s + 2) * sub], preferred_element_type=f32)
        ids = ids_ref[:, span] - i * rows
        weight = jnp.where(here == ids, 0.0, jnp.exp(logits))
        row_sum[:, span] += jnp.sum(weight.reshape(rows // 8, 8, sub), axis=0)
        weight = weight.astype(bf16)
        exp_ref[:, span] = weight
        total[:, span] += jnp.dot(turned, weight, preferred_element_type=f32)
        if s + 1 < parts:
            logits = later

    @pl.when(i == pl.num_programs(0) - 1)
    def _():
        pull_ref[...] = total[...].astype(bf16).T
        found = found_ref[...]
        target_cos = jnp.sum(turned_emb[...].astype(f32) * found, axis=0, keepdims=True) * (1.0 / logit_scale)
        sums_ref[...] = jnp.sum(row_sum[...], axis=0, keepdims=True)
        stat_ref[...] = target_cos


def exponentials(x, ids, found, low, turned, rows=512, sub=256):
    samples, depth = x.shape
    count = low.shape[0]
    fixed = lambda i: (0, 0)
    return pl.pallas_call(
        functools.partial(logits_kernel, sub),
        grid=(count // rows,),
        in_specs=[
            pl.BlockSpec((samples, depth), fixed),
            pl.BlockSpec((1, samples), fixed),
            pl.BlockSpec((depth, samples), fixed),
            pl.BlockSpec((rows, depth), lambda i: (i, 0)),
            pl.BlockSpec((depth, rows), lambda i: (0, i)),
        ],
        out_specs=[
            pl.BlockSpec((rows, samples), lambda i: (i, 0)),
            pl.BlockSpec((1, samples), fixed),
            pl.BlockSpec((samples, depth), fixed),
            pl.BlockSpec((1, samples), fixed),
            pl.BlockSpec((samples, depth), fixed),
        ],
        out_shape=[
            jax.ShapeDtypeStruct((count, samples), bf16),
            jax.ShapeDtypeStruct((1, samples), f32),
            jax.ShapeDtypeStruct((samples, depth), bf16),
            jax.ShapeDtypeStruct((1, samples), f32),
            jax.ShapeDtypeStruct((samples, depth), bf16),
        ],
        scratch_shapes=[
            pltpu.VMEM((depth, samples), bf16),
            pltpu.VMEM((depth, samples), f32),
            pltpu.VMEM((8, samples), f32),
        ],
        compiler_params=pltpu.CompilerParams(vmem_limit_bytes=36 * MIB),
        cost_estimate=pl.CostEstimate(
            flops=4 * count * depth * samples, bytes_accessed=4 * count * depth, transcendentals=count * samples
        ),
        name="exponentials",
    )(x, ids, found, low, turned)


def push_kernel(base, final, ids_ref, patch_ref, emb_ref, exp_ref, *refs):
    i = pl.program_id(0)
    rows = exp_ref.shape[0]
    ids = ids_ref[...] - (base + i) * rows
    hit = lax.broadcasted_iota(jnp.int32, exp_ref.shape, 0) == ids
    weight = jnp.where(hit, patch_ref[...], exp_ref[...].astype(f32)).astype(bf16)
    push = jnp.dot(weight, emb_ref[...], preferred_element_type=f32)
    if final:
        c_ref, other_ref, out_ref = refs
        push = push + other_ref[...].astype(f32)
        block = c_ref[...].astype(f32)
        inv = inverse_norm(block, 1)
        unit = block * inv
        push = (push - unit * jnp.sum(push * unit, axis=1, keepdims=True)) * inv
        out_ref[...] = push.astype(bf16)
    else:
        (out_ref,) = refs
        out_ref[...] = push.astype(bf16)


def pushed(ids, patch, emb, exps, half, centers=None, other=None, rows=512):
    samples, depth = emb.shape
    count = exps.shape[0] // 2
    base = half * (count // rows)
    final = centers is not None
    fixed = lambda i: (0, 0)
    step = lambda i: (i, 0)
    extra = (centers, other) if final else ()
    return pl.pallas_call(
        functools.partial(push_kernel, base, final),
        grid=(count // rows,),
        in_specs=[
            pl.BlockSpec((1, samples), fixed),
            pl.BlockSpec((1, samples), fixed),
            pl.BlockSpec((samples, depth), fixed),
            pl.BlockSpec((rows, samples), lambda i: (base + i, 0)),
        ]
        + [pl.BlockSpec((rows, depth), step)] * len(extra),
        out_specs=pl.BlockSpec((rows, depth), step),
        out_shape=jax.ShapeDtypeStruct((count, depth), bf16),
        compiler_params=pltpu.CompilerParams(vmem_limit_bytes=24 * MIB),
        cost_estimate=pl.CostEstimate(
            flops=2 * count * depth * samples, bytes_accessed=2 * count * samples, transcendentals=0
        ),
        name=f"push_{half}",
    )(ids, patch, emb, exps, *extra)


def on_device(features, fc_weight, centers, labels):
    own, wide = features.shape
    class_rows, depth = centers.shape
    chips = lax.axis_size(CHIP)
    chip = lax.axis_index(CHIP)
    core = lax.axis_index(CORE)
    samples = chips * own

    other_centers = swapped(centers)
    embedded = jnp.dot(features, fc_weight, preferred_element_type=f32).astype(bf16)
    x = from_chips(embedded).reshape(samples, depth)

    by_core = labels.reshape(chips, 2, own)
    my_labels = jnp.where(core == 0, by_core[:, 0], by_core[:, 1]).reshape(1, samples)
    local = my_labels - chip * (2 * class_rows)
    inside = (local >= 0) & (local < 2 * class_rows)
    turned_ids = jnp.where(core == 0, local, (local + class_rows) % (2 * class_rows))
    ids = jnp.where(inside, turned_ids, -1)

    low, turned, found_a = prepared_centers(centers, ids, None, 0, 2)
    low, turned, found_b = prepared_centers(other_centers, ids, (low, turned), 1, 2)
    found = found_a + found_b

    split = features.reshape(own, chips, 2, wide // (2 * chips))
    mine = jnp.where(core == 0, split[:, :, 0], split[:, :, 1])
    theirs = jnp.where(core == 0, split[:, :, 1], split[:, :, 0])
    fcols = mine.shape[-1]
    pad = ((0, 0), (0, 0), (0, 128 - fcols))
    cargo = jnp.concatenate(
        [
            found.astype(bf16).T.reshape(chips, own, depth),
            jnp.pad(mine.swapaxes(0, 1), pad),
            jnp.pad(theirs.swapaxes(0, 1), pad),
        ],
        axis=2,
    )
    cargo = to_chips(cargo)

    exps, part_sums, pull, target_cos, emb_low = exponentials(x, ids, found, low, turned)
    is_here = ids >= 0
    margined, slope = margin(target_cos)
    target_exp = jnp.exp(logit_scale * margined)
    part_sums = part_sums + jnp.where(is_here, target_exp, 0.0)

    pulls = to_chips(pull.reshape(chips, own, depth))
    sums = jnp.sum(from_chips(part_sums), axis=0)

    patch = slope * (target_exp - sums)
    scaled = (emb_low.astype(f32) * (logit_scale / sums.reshape(samples, 1))).astype(bf16)
    other_push = swapped(pushed(ids, patch, scaled, exps, 1))
    grad_centers = pushed(ids, patch, scaled, exps, 0, centers, other_push)

    own_float = embedded.astype(f32)
    inv_emb = inverse_norm(own_float, 1)
    emb_dir = own_float * inv_emb
    own_target = jnp.sum(cargo[:, :, :depth].astype(f32), axis=0)
    own_cos = jnp.sum(emb_dir.astype(bf16).astype(f32) * own_target, axis=1, keepdims=True)
    own_margined, own_slope = margin(own_cos)
    own_logit = logit_scale * own_margined
    own_sums = lax.dynamic_slice_in_dim(sums.reshape(samples), chip * own, own).reshape(own, 1)
    loss = (jnp.log(own_sums) - own_logit).reshape(own)
    own_pull = jnp.sum(pulls.astype(f32), axis=0)
    at_target = logit_scale * own_slope * (jnp.exp(own_logit) / own_sums - 1.0)
    grad_dir = own_pull * (logit_scale / own_sums) + at_target * own_target
    grad_emb = (
        (grad_dir - emb_dir * jnp.sum(grad_dir * emb_dir, axis=1, keepdims=True)) * inv_emb
    ).astype(bf16)

    grads = from_chips(grad_emb).reshape(samples, depth)
    columns = cargo[:, :, depth:].reshape(samples, 256)
    both = lax.dot_general(columns, grads, (((0,), (0,)), ((), ())), preferred_element_type=f32)
    grad_fc = both[:fcols] + swapped(both[128 : 128 + fcols])
    return (loss, grad_centers, grad_fc)


def solution(mesh):
    torus = Mesh(mesh.devices.reshape(4, 4, 4, 2), CLS)
    placed = (P(CLS, None), P(), P(CLS, None), P())
    return jax.shard_map(
        on_device,
        mesh=torus,
        in_specs=placed,
        out_specs=(P(CLS), P(CLS, None), P(CLS, None)),
        check_vma=False,
    )
```

```python
import functools
import math

import jax
import jax.numpy as jnp
from jax import lax
from jax.experimental import pallas as pl
from jax.experimental.pallas import tpu as pltpu
from jax.sharding import Mesh
from jax.sharding import PartitionSpec as P


CLS = ("cls_0", "cls_1", "cls_2", "cls_3")
CHIP = ("cls_0", "cls_1", "cls_2")
CORE = "cls_3"

logit_scale = 64.0
cos_margin = math.cos(0.5)
sin_margin = math.sin(0.5)
epsilon = 1e-06

f32 = jnp.float32
bf16 = jnp.bfloat16


def swapped(x):
    return lax.ppermute(x, CORE, [(0, 1), (1, 0)])


def to_chips(x):
    return lax.all_to_all(x, CHIP, split_axis=0, concat_axis=0, tiled=True)


def from_chips(x):
    copies = jnp.broadcast_to(x, (lax.axis_size(CHIP), *x.shape))
    return lax.all_to_all(copies, CHIP, split_axis=0, concat_axis=0, tiled=True)


def inverse_norm(values, axis):
    return lax.rsqrt(jnp.sum(values * values, axis=axis, keepdims=True) + epsilon)


def margin(target_cos):
    target_sine = jnp.sqrt(1.0 - target_cos * target_cos)
    margined = target_cos * cos_margin - target_sine * sin_margin
    slope = cos_margin + sin_margin * target_cos / target_sine
    return margined, slope


def targets_kernel(steps, ids_ref, own_ref, other_ref, found_ref, wide_ids, total):
    i = pl.program_id(0)
    rows = own_ref.shape[0]
    samples = found_ref.shape[0]

    @pl.when(i == 0)
    def _():
        wide_ids[...] = jnp.broadcast_to(ids_ref[...], (128, samples)).T
        total[...] = jnp.zeros_like(total)

    ids = jnp.concatenate([wide_ids[...] - i * rows] * (rows // 128), axis=1)
    hit = jnp.where(lax.broadcasted_iota(jnp.int32, (samples, rows), 1) == ids, 1.0, 0.0).astype(bf16)

    @pl.when(i < steps)
    def _():
        total[...] += jnp.dot(hit, own_ref[...], preferred_element_type=f32)

    @pl.when(i >= steps)
    def _():
        total[...] += jnp.dot(hit, other_ref[...], preferred_element_type=f32)

    @pl.when(i == 2 * steps - 1)
    def _():
        found_ref[...] = total[...].astype(bf16)


def halves(rows, depth, steps):
    return [
        pl.BlockSpec((rows, depth), lambda i: (jnp.minimum(i, steps - 1), 0)),
        pl.BlockSpec((rows, depth), lambda i: (jnp.maximum(i - steps, 0), 0)),
    ]


def target_rows(ids, own, other, rows=512):
    count, depth = own.shape
    samples = ids.shape[1]
    steps = count // rows
    fixed = lambda i: (0, 0)
    return pl.pallas_call(
        functools.partial(targets_kernel, steps),
        grid=(2 * steps,),
        in_specs=[pl.BlockSpec((1, samples), fixed)] + halves(rows, depth, steps),
        out_specs=pl.BlockSpec((samples, depth), fixed),
        out_shape=jax.ShapeDtypeStruct((samples, depth), bf16),
        scratch_shapes=[pltpu.VMEM((samples, 128), jnp.int32), pltpu.VMEM((samples, depth), f32)],
        cost_estimate=pl.CostEstimate(
            flops=4 * count * depth * samples, bytes_accessed=4 * count * depth, transcendentals=0
        ),
        name="targets",
    )(ids, own, other)


def row_of(values):
    part = values[:, :128]
    for k in range(1, values.shape[1] // 128):
        part = part + values[:, k * 128 : (k + 1) * 128]
    return jnp.sum(part.T, axis=0, keepdims=True)


def exp_kernel(steps, sub, ids_ref, x_ref, found_ref, own_ref, other_ref, exp_ref, low_ref, emb_ref, goal_ref,
               sums_ref, cos_ref, wide_ids, scaled, row_sum):
    i = pl.program_id(0)
    rows = own_ref.shape[0]
    samples = x_ref.shape[0]

    @pl.when(i == 0)
    def _():
        wide_ids[...] = jnp.broadcast_to(ids_ref[...], (128, samples)).T
        x = x_ref[...].astype(f32)
        emb = (x * inverse_norm(x, 1)).astype(bf16)
        emb_ref[...] = emb
        scaled[...] = (emb * logit_scale).astype(bf16)
        row_sum[...] = jnp.zeros_like(row_sum)

    block = jnp.where(i < steps, own_ref[...], other_ref[...]).astype(f32)
    low = (block * inverse_norm(block, 1)).astype(bf16)
    low_ref[...] = low
    columns = lax.broadcasted_iota(jnp.int32, (sub, rows), 1)
    parts = samples // sub

    def products(s):
        return lax.dot_general(
            scaled[s * sub : (s + 1) * sub, :], low, (((1,), (1,)), ((), ())), preferred_element_type=f32
        )

    logits = products(0)
    for s in range(parts):
        span = slice(s * sub, (s + 1) * sub)
        later = products(s + 1) if s + 1 < parts else None
        ids = jnp.concatenate([wide_ids[span, :] - i * rows] * (rows // 128), axis=1)
        weight = jnp.where(columns == ids, 0.0, jnp.exp(logits))
        part = weight[:, :128]
        for k in range(1, rows // 128):
            part = part + weight[:, k * 128 : (k + 1) * 128]
        row_sum[span, :] += part
        exp_ref[span, :] = weight.astype(bf16)
        logits = later

    @pl.when(i == 2 * steps - 1)
    def _():
        found = found_ref[...].astype(f32)
        goal = (found * inverse_norm(found, 1)).astype(bf16)
        goal_ref[...] = goal
        target_cos = row_of(goal.astype(f32) * scaled[...].astype(f32)) * (1.0 / logit_scale)
        cos_ref[...] = target_cos
        margined, _ = margin(target_cos)
        here = jnp.where(ids_ref[...] >= 0, jnp.exp(logit_scale * margined), 0.0)
        sums_ref[...] = row_of(row_sum[...]) + here


def exponentials(ids, x, found, own, other, rows=512, sub=256):
    samples, depth = x.shape
    count = own.shape[0]
    steps = count // rows
    fixed = lambda i: (0, 0)
    return pl.pallas_call(
        functools.partial(exp_kernel, steps, sub),
        grid=(2 * steps,),
        in_specs=[
            pl.BlockSpec((1, samples), fixed),
            pl.BlockSpec((samples, depth), fixed),
            pl.BlockSpec((samples, depth), fixed),
        ]
        + halves(rows, depth, steps),
        out_specs=[
            pl.BlockSpec((samples, rows), lambda i: (0, i)),
            pl.BlockSpec((rows, depth), lambda i: (i, 0)),
            pl.BlockSpec((samples, depth), fixed),
            pl.BlockSpec((samples, depth), fixed),
            pl.BlockSpec((1, samples), fixed),
            pl.BlockSpec((1, samples), fixed),
        ],
        out_shape=[
            jax.ShapeDtypeStruct((samples, 2 * count), bf16),
            jax.ShapeDtypeStruct((2 * count, depth), bf16),
            jax.ShapeDtypeStruct((samples, depth), bf16),
            jax.ShapeDtypeStruct((samples, depth), bf16),
            jax.ShapeDtypeStruct((1, samples), f32),
            jax.ShapeDtypeStruct((1, samples), f32),
        ],
        scratch_shapes=[
            pltpu.VMEM((samples, 128), jnp.int32),
            pltpu.VMEM((samples, depth), bf16),
            pltpu.VMEM((samples, 128), f32),
        ],
        cost_estimate=pl.CostEstimate(
            flops=4 * count * depth * samples,
            bytes_accessed=8 * count * depth,
            transcendentals=2 * count * samples,
        ),
        name="exponentials",
    )(ids, x, found, own, other)


def pull_kernel(exp_ref, low_ref, out_ref):
    i = pl.program_id(0)
    product = jnp.dot(exp_ref[...], low_ref[...], preferred_element_type=f32)

    @pl.when(i == 0)
    def _():
        out_ref[...] = product

    @pl.when(i > 0)
    def _():
        out_ref[...] += product


def pulled(exps, low, rows=1024):
    samples = exps.shape[0]
    count, depth = low.shape
    return pl.pallas_call(
        pull_kernel,
        grid=(count // rows,),
        in_specs=[
            pl.BlockSpec((samples, rows), lambda i: (0, i)),
            pl.BlockSpec((rows, depth), lambda i: (i, 0)),
        ],
        out_specs=pl.BlockSpec((samples, depth), lambda i: (0, 0)),
        out_shape=jax.ShapeDtypeStruct((samples, depth), f32),
        cost_estimate=pl.CostEstimate(
            flops=2 * count * depth * samples, bytes_accessed=2 * count * (depth + samples), transcendentals=0
        ),
        name="pull",
    )(exps, low)


def push_kernel(base, final, ids_ref, patch_ref, emb_ref, exp_ref, *refs):
    i = pl.program_id(0)
    samples, rows = exp_ref.shape
    if final:
        c_ref, other_ref, out_ref, wide_ids, wide_patch = refs
    else:
        out_ref, wide_ids, wide_patch = refs

    @pl.when(i == 0)
    def _():
        wide_ids[...] = jnp.broadcast_to(ids_ref[...], (128, samples)).T
        wide_patch[...] = jnp.broadcast_to(patch_ref[...], (128, samples)).T

    ids = jnp.concatenate([wide_ids[...] - (base + i) * rows] * (rows // 128), axis=1)
    patch = jnp.concatenate([wide_patch[...]] * (rows // 128), axis=1)
    hit = lax.broadcasted_iota(jnp.int32, exp_ref.shape, 1) == ids
    weight = jnp.where(hit, patch, exp_ref[...].astype(f32)).astype(bf16)
    push = lax.dot_general(weight, emb_ref[...], (((0,), (0,)), ((), ())), preferred_element_type=f32)
    if final:
        push = push + other_ref[...].astype(f32)
        block = c_ref[...].astype(f32)
        inv = inverse_norm(block, 1)
        unit = block * inv
        push = (push - unit * jnp.sum(push * unit, axis=1, keepdims=True)) * inv
    out_ref[...] = push.astype(bf16)


def pushed(ids, patch, emb, exps, half, centers=None, other=None, rows=512):
    samples, depth = emb.shape
    count = exps.shape[1] // 2
    base = half * (count // rows)
    final = centers is not None
    fixed = lambda i: (0, 0)
    step = lambda i: (i, 0)
    extra = (centers, other) if final else ()
    return pl.pallas_call(
        functools.partial(push_kernel, base, final),
        grid=(count // rows,),
        in_specs=[
            pl.BlockSpec((1, samples), fixed),
            pl.BlockSpec((1, samples), fixed),
            pl.BlockSpec((samples, depth), fixed),
            pl.BlockSpec((samples, rows), lambda i: (0, base + i)),
        ]
        + [pl.BlockSpec((rows, depth), step)] * len(extra),
        out_specs=pl.BlockSpec((rows, depth), step),
        out_shape=jax.ShapeDtypeStruct((count, depth), bf16),
        scratch_shapes=[pltpu.VMEM((samples, 128), jnp.int32), pltpu.VMEM((samples, 128), f32)],
        cost_estimate=pl.CostEstimate(
            flops=2 * count * depth * samples, bytes_accessed=2 * count * samples, transcendentals=0
        ),
    )(ids, patch, emb, exps, *extra)


def step(features, fc_weight, centers, labels):
    own, wide = features.shape
    class_rows, depth = centers.shape
    chips = lax.axis_size(CHIP)
    chip = lax.axis_index(CHIP)
    core = lax.axis_index(CORE)
    samples = chips * own

    other_centers = swapped(centers)
    embedded = jnp.dot(features, fc_weight, preferred_element_type=f32).astype(bf16)
    x = from_chips(embedded).reshape(samples, depth)

    by_core = labels.reshape(chips, 2, own)
    my_labels = jnp.where(core == 0, by_core[:, 0], by_core[:, 1]).reshape(1, samples)
    local = my_labels - chip * (2 * class_rows)
    inside = (local >= 0) & (local < 2 * class_rows)
    turned_ids = jnp.where(core == 0, local, (local + class_rows) % (2 * class_rows))
    ids = jnp.where(inside, turned_ids, -1)

    split = features.reshape(own, chips, 2, wide // (2 * chips))
    mine = jnp.where(core == 0, split[:, :, 0], split[:, :, 1])
    theirs = jnp.where(core == 0, split[:, :, 1], split[:, :, 0])
    fcols = mine.shape[-1]
    pad = ((0, 0), (0, 0), (0, 128 - fcols))
    cargo = jnp.concatenate([jnp.pad(mine.swapaxes(0, 1), pad), jnp.pad(theirs.swapaxes(0, 1), pad)], axis=2)

    found = target_rows(ids, centers, other_centers)
    exps, low, emb_low, goal, part_sums, target_cos = exponentials(ids, x, found, centers, other_centers)
    margined, slope = margin(target_cos)
    target_exp = jnp.exp(logit_scale * margined)
    goal_logit = jnp.where(ids >= 0, logit_scale * margined, 0.0).reshape(chips, 1, own)
    report = jnp.concatenate(
        [jnp.broadcast_to(part_sums, (chips, 1, samples)), jnp.pad(goal_logit, ((0, 0), (0, 0), (0, 128 - own)))],
        axis=2,
    )
    report = to_chips(report)
    pull = pulled(exps, low)
    report = jnp.sum(report, axis=0)
    sums = report[:, :samples]

    patch = slope * (target_exp - sums)
    scale = logit_scale / sums
    scale_column = scale.reshape(samples, 1)
    at_target = jnp.where(ids >= 0, scale * patch, 0.0).reshape(samples, 1)
    pull = (pull * scale_column + at_target * goal.astype(f32)).astype(bf16)
    scaled = (emb_low.astype(f32) * scale_column).astype(bf16)
    parcel = jnp.concatenate([pull.reshape(chips, own, depth), cargo], axis=2)
    parcel = to_chips(parcel)

    other_push = pushed(ids, patch, scaled, exps, 1)
    other_push = swapped(other_push)
    grad_centers = pushed(ids, patch, scaled, exps, 0, centers, other_push)

    own_float = embedded.astype(f32)
    inv_emb = inverse_norm(own_float, 1)
    emb_dir = own_float * inv_emb
    grad_dir = jnp.sum(parcel[:, :, :depth].astype(f32), axis=0)
    grad_emb = (
        (grad_dir - emb_dir * jnp.sum(grad_dir * emb_dir, axis=1, keepdims=True)) * inv_emb
    ).astype(bf16)
    grads = from_chips(grad_emb).reshape(samples, depth)

    columns = parcel[:, :, depth:].reshape(samples, 256)
    both = lax.dot_general(columns, grads, (((0,), (0,)), ((), ())), preferred_element_type=f32)
    theirs_fc = swapped(both[128 : 128 + fcols])
    grad_fc = both[:fcols] + theirs_fc
    own_sums = lax.dynamic_slice_in_dim(sums.reshape(samples), chip * own, own)
    loss = jnp.log(own_sums) - report[0, samples : samples + own]
    return (loss, grad_centers, grad_fc)


def solution(mesh):
    torus = Mesh(mesh.devices.reshape(4, 4, 4, 2), CLS)
    placed = (P(CLS, None), P(), P(CLS, None), P())
    return jax.shard_map(
        step,
        mesh=torus,
        in_specs=placed,
        out_specs=(P(CLS), P(CLS, None), P(CLS, None)),
        check_vma=False,
    )
```

```python
import functools
import math

import jax
import jax.numpy as jnp
from jax import lax
from jax.experimental import pallas as pl
from jax.experimental.pallas import tpu as pltpu
from jax.sharding import Mesh
from jax.sharding import PartitionSpec as P


CLS = ("cls_0", "cls_1", "cls_2", "cls_3")
CHIP = ("cls_0", "cls_1", "cls_2")
CORE = "cls_3"

logit_scale = 64.0
cos_margin = math.cos(0.5)
sin_margin = math.sin(0.5)
epsilon = 1e-06

f32 = jnp.float32
bf16 = jnp.bfloat16


def swapped(x):
    return lax.ppermute(x, CORE, [(0, 1), (1, 0)])


def to_chips(x):
    return lax.all_to_all(x, CHIP, split_axis=0, concat_axis=0, tiled=True)


def from_chips(x):
    copies = jnp.broadcast_to(x, (lax.axis_size(CHIP), *x.shape))
    return lax.all_to_all(copies, CHIP, split_axis=0, concat_axis=0, tiled=True)


def inverse_norm(values, axis):
    return lax.rsqrt(jnp.sum(values * values, axis=axis, keepdims=True) + epsilon)


def margin(target_cos):
    target_sine = jnp.sqrt(1.0 - target_cos * target_cos)
    margined = target_cos * cos_margin - target_sine * sin_margin
    slope = cos_margin + sin_margin * target_cos / target_sine
    return margined, slope


ANY = pl.BlockSpec(memory_space=pl.ANY)
VMEM = pl.BlockSpec(memory_space=pltpu.VMEM)
SMEM = pl.BlockSpec(memory_space=pltpu.SMEM)


def targets_kernel(batch, ids_ref, busy_ref, own_ref, other_ref, goal_ref, centers, found, sems):
    count, depth = own_ref.shape
    copies = [
        pltpu.make_async_copy(part, centers.at[pl.ds(k * count, count)], sems.at[k])
        for k, part in enumerate((own_ref, other_ref))
    ]
    for copy in copies:
        copy.start()
    found[...] = jnp.zeros_like(found)
    for copy in copies:
        copy.wait()
    spot = lax.broadcasted_iota(jnp.int32, (16, depth), 0)

    def group(g, carry):
        @pl.when(busy_ref[g] >= 0)
        def _():
            def sample(b, carry):
                at = g * batch + b
                row = ids_ref[at]

                @pl.when(row >= 0)
                def _():
                    near = centers[pl.ds(pl.multiple_of(row // 16 * 16, 16), 16), :].astype(f32)
                    found[pl.ds(at, 1), :] = jnp.sum(jnp.where(spot == row % 16, near, 0.0), axis=0, keepdims=True)

                return carry

            lax.fori_loop(0, batch, sample, 0)

        return carry

    lax.fori_loop(0, busy_ref.shape[0], group, 0)
    rows = found[...]
    goal_ref[...] = (rows * inverse_norm(rows, 1)).astype(bf16)


def target_directions(ids, batch, own, other):
    count, depth = own.shape
    samples = ids.shape[0]
    busy = jnp.max(ids.reshape(samples // batch, batch), axis=1)
    return pl.pallas_call(
        functools.partial(targets_kernel, batch),
        in_specs=[SMEM, SMEM, ANY, ANY],
        out_specs=VMEM,
        out_shape=jax.ShapeDtypeStruct((samples, depth), bf16),
        scratch_shapes=[
            pltpu.VMEM((2 * count, depth), bf16),
            pltpu.VMEM((samples, depth), f32),
            pltpu.SemaphoreType.DMA((2,)),
        ],
        cost_estimate=pl.CostEstimate(
            flops=2 * count * depth * samples, bytes_accessed=4 * count * depth, transcendentals=0
        ),
        name="targets",
    )(ids, busy, own, other)


def row_of(values):
    part = values[:, :128]
    for k in range(1, values.shape[1] // 128):
        part = part + values[:, k * 128 : (k + 1) * 128]
    return jnp.sum(part.T, axis=0, keepdims=True)


def exp_kernel(steps, early, lanes, ids_ref, x_ref, goal_ref, own_ref, other_ref, exp_ref, low_ref, pull_ref, emb_ref,
               sums_ref, cos_ref, wide_ids, scaled, row_sum, total):
    i = pl.program_id(0)
    rows = own_ref.shape[0]
    samples = x_ref.shape[0]
    sub = samples // lanes

    @pl.when(i == 0)
    def _():
        wide_ids[...] = jnp.broadcast_to(ids_ref[...], (128, samples)).T
        x = x_ref[...].astype(f32)
        emb = (x * inverse_norm(x, 1)).astype(bf16)
        emb_ref[...] = emb
        scaled[...] = (emb * logit_scale).astype(bf16)
        row_sum[...] = jnp.zeros_like(row_sum)
        total[...] = jnp.zeros_like(total)

    def chunk(with_pull):
        block = jnp.where(i < steps, own_ref[...], other_ref[...]).astype(f32)
        low_ref[...] = (block * inverse_norm(block, 1)).astype(bf16)
        columns = lax.broadcasted_iota(jnp.int32, (sub, 128), 1)

        def products(m):
            return lax.dot_general(
                scaled[m * sub : (m + 1) * sub, :],
                low_ref[...],
                (((1,), (1,)), ((), ())),
                preferred_element_type=f32,
            )

        logits = products(0)
        for m in range(lanes):
            later = products(m + 1) if m + 1 < lanes else None
            span = slice(m * sub, (m + 1) * sub)
            ids = wide_ids[span, :] - i * rows
            part = None
            for t in range(rows // 128):
                weight = jnp.exp(logits[:, t * 128 : (t + 1) * 128])
                weight = jnp.where(columns + t * 128 == ids, 0.0, weight)
                part = weight if part is None else part + weight
                exp_ref[span, t * 128 : (t + 1) * 128] = weight.astype(bf16)
            row_sum[span, :] += part
            if with_pull:
                total[span, :] += jnp.dot(exp_ref[span, :], low_ref[...], preferred_element_type=f32)
            logits = later

    @pl.when(i < early)
    def _():
        chunk(True)

    @pl.when(i >= early)
    def _():
        chunk(False)

    @pl.when(i == early)
    def _():
        pull_ref[...] = total[...]

    @pl.when(i == 2 * steps - 1)
    def _():
        target_cos = row_of(goal_ref[...].astype(f32) * scaled[...].astype(f32)) * (1.0 / logit_scale)
        cos_ref[...] = target_cos
        margined, _ = margin(target_cos)
        here = jnp.where(ids_ref[...] >= 0, jnp.exp(logit_scale * margined), 0.0)
        sums_ref[...] = row_of(row_sum[...]) + here


def exponentials(ids, x, goal, own, other, early, rows=1024, lanes=2):
    samples, depth = x.shape
    count = own.shape[0]
    steps = count // rows
    late = 2 * steps - early
    fixed = lambda i: (0, 0)
    return pl.pallas_call(
        functools.partial(exp_kernel, steps, early, lanes),
        grid=(2 * steps,),
        in_specs=[
            pl.BlockSpec((1, samples), fixed),
            pl.BlockSpec((samples, depth), fixed),
            pl.BlockSpec((samples, depth), fixed),
            pl.BlockSpec((rows, depth), lambda i: (jnp.minimum(i, steps - 1), 0)),
            pl.BlockSpec((rows, depth), lambda i: (jnp.maximum(i - steps, 0), 0)),
        ],
        out_specs=[
            pl.BlockSpec((samples, rows), lambda i: (0, i)),
            pl.BlockSpec((rows, depth), lambda i: (jnp.maximum(i - early, 0), 0)),
            pl.BlockSpec((samples, depth), fixed),
            pl.BlockSpec((samples, depth), fixed),
            pl.BlockSpec((1, samples), fixed),
            pl.BlockSpec((1, samples), fixed),
        ],
        out_shape=[
            jax.ShapeDtypeStruct((samples, 2 * count), bf16),
            jax.ShapeDtypeStruct((late * rows, depth), bf16),
            jax.ShapeDtypeStruct((samples, depth), f32),
            jax.ShapeDtypeStruct((samples, depth), bf16),
            jax.ShapeDtypeStruct((1, samples), f32),
            jax.ShapeDtypeStruct((1, samples), f32),
        ],
        scratch_shapes=[
            pltpu.VMEM((samples, 128), jnp.int32),
            pltpu.VMEM((samples, depth), bf16),
            pltpu.VMEM((samples, 128), f32),
            pltpu.VMEM((samples, depth), f32),
        ],
        cost_estimate=pl.CostEstimate(
            flops=4 * count * depth * samples,
            bytes_accessed=8 * count * depth,
            transcendentals=2 * count * samples,
        ),
        name="exponentials",
    )(ids, x, goal, own, other)


def pull_kernel(early, rows, exp_ref, low_ref, start_ref, out_ref, exps, lows, exp_sems, low_sems, start_sem):
    steps = low_ref.shape[0] // rows
    start = pltpu.make_async_copy(start_ref, out_ref, start_sem)

    def fetch(i, slot):
        return (
            pltpu.make_async_copy(
                exp_ref.at[:, pl.ds((early + i) * rows, rows)], exps.at[slot], exp_sems.at[slot]
            ),
            pltpu.make_async_copy(low_ref.at[pl.ds(i * rows, rows)], lows.at[slot], low_sems.at[slot]),
        )

    for i in range(steps):
        for copy in fetch(i, i):
            copy.start()
        if i == 0:
            start.start()
    for i in range(steps):
        for copy in fetch(i, i):
            copy.wait()
        if i == 0:
            start.wait()
        out_ref[...] += jnp.dot(exps[i], lows[i], preferred_element_type=f32)


def pulled(exps, low, start, early, rows=1024):
    samples = exps.shape[0]
    count, depth = low.shape
    steps = count // rows
    return pl.pallas_call(
        functools.partial(pull_kernel, early, rows),
        in_specs=[ANY, ANY, ANY],
        out_specs=VMEM,
        out_shape=jax.ShapeDtypeStruct((samples, depth), f32),
        scratch_shapes=[
            pltpu.VMEM((steps, samples, rows), bf16),
            pltpu.VMEM((steps, rows, depth), bf16),
            pltpu.SemaphoreType.DMA((steps,)),
            pltpu.SemaphoreType.DMA((steps,)),
            pltpu.SemaphoreType.DMA,
        ],
        cost_estimate=pl.CostEstimate(
            flops=2 * count * depth * samples, bytes_accessed=2 * count * (depth + samples), transcendentals=0
        ),
        name="pull",
    )(exps, low, start)


def push_kernel(base, final, ids_ref, patch_ref, emb_ref, exp_ref, *refs):
    i = pl.program_id(0)
    samples, rows = exp_ref.shape
    if final:
        c_ref, other_ref, out_ref, wide_ids, wide_patch = refs
    else:
        out_ref, wide_ids, wide_patch = refs

    @pl.when(i == 0)
    def _():
        wide_ids[...] = jnp.broadcast_to(ids_ref[...], (128, samples)).T
        wide_patch[...] = jnp.broadcast_to(patch_ref[...], (128, samples)).T

    ids = jnp.concatenate([wide_ids[...] - (base + i) * rows] * (rows // 128), axis=1)
    patch = jnp.concatenate([wide_patch[...]] * (rows // 128), axis=1)
    hit = lax.broadcasted_iota(jnp.int32, exp_ref.shape, 1) == ids
    weight = jnp.where(hit, patch, exp_ref[...].astype(f32)).astype(bf16)
    push = lax.dot_general(weight, emb_ref[...], (((0,), (0,)), ((), ())), preferred_element_type=f32)
    if final:
        push = push + other_ref[...].astype(f32)
        block = c_ref[...].astype(f32)
        inv = inverse_norm(block, 1)
        unit = block * inv
        push = (push - unit * jnp.sum(push * unit, axis=1, keepdims=True)) * inv
    out_ref[...] = push.astype(bf16)


def pushed(ids, patch, emb, exps, half, centers=None, other=None, rows=512):
    samples, depth = emb.shape
    count = exps.shape[1] // 2
    base = half * (count // rows)
    final = centers is not None
    fixed = lambda i: (0, 0)
    step = lambda i: (i, 0)
    extra = (centers, other) if final else ()
    return pl.pallas_call(
        functools.partial(push_kernel, base, final),
        grid=(count // rows,),
        in_specs=[
            pl.BlockSpec((1, samples), fixed),
            pl.BlockSpec((1, samples), fixed),
            pl.BlockSpec((samples, depth), fixed),
            pl.BlockSpec((samples, rows), lambda i: (0, base + i)),
        ]
        + [pl.BlockSpec((rows, depth), step)] * len(extra),
        out_specs=pl.BlockSpec((rows, depth), step),
        out_shape=jax.ShapeDtypeStruct((count, depth), bf16),
        scratch_shapes=[pltpu.VMEM((samples, 128), jnp.int32), pltpu.VMEM((samples, 128), f32)],
        cost_estimate=pl.CostEstimate(
            flops=2 * count * depth * samples, bytes_accessed=2 * count * samples, transcendentals=0
        ),
    )(ids, patch, emb, exps, *extra)


def step(features, fc_weight, centers, labels):
    own, wide = features.shape
    class_rows, depth = centers.shape
    chips = lax.axis_size(CHIP)
    chip = lax.axis_index(CHIP)
    core = lax.axis_index(CORE)
    samples = chips * own

    other_centers = swapped(centers)
    embedded = jnp.dot(features, fc_weight, preferred_element_type=f32).astype(bf16)
    x = from_chips(embedded).reshape(samples, depth)

    by_core = labels.reshape(chips, 2, own)
    my_labels = jnp.where(core == 0, by_core[:, 0], by_core[:, 1]).reshape(1, samples)
    local = my_labels - chip * (2 * class_rows)
    inside = (local >= 0) & (local < 2 * class_rows)
    turned_ids = jnp.where(core == 0, local, (local + class_rows) % (2 * class_rows))
    ids = jnp.where(inside, turned_ids, -1)

    split = features.reshape(own, chips, 2, wide // (2 * chips))
    mine = jnp.where(core == 0, split[:, :, 0], split[:, :, 1])
    theirs = jnp.where(core == 0, split[:, :, 1], split[:, :, 0])
    fcols = mine.shape[-1]
    pad = ((0, 0), (0, 0), (0, 128 - fcols))
    cargo = jnp.concatenate([jnp.pad(mine.swapaxes(0, 1), pad), jnp.pad(theirs.swapaxes(0, 1), pad)], axis=2)

    goal = target_directions(ids.reshape(samples), own, centers, other_centers)
    early = 6
    exps, low, pull, emb_low, part_sums, target_cos = exponentials(ids, x, goal, centers, other_centers, early)
    margined, slope = margin(target_cos)
    target_exp = jnp.exp(logit_scale * margined)
    goal_logit = jnp.where(ids >= 0, logit_scale * margined, 0.0).reshape(chips, 1, own)
    report = jnp.concatenate(
        [jnp.broadcast_to(part_sums, (chips, 1, samples)), jnp.pad(goal_logit, ((0, 0), (0, 0), (0, 128 - own)))],
        axis=2,
    )
    report = to_chips(report)
    pull = pulled(exps, low, pull, early)
    report = jnp.sum(report, axis=0)
    sums = report[:, :samples]

    patch = slope * (target_exp - sums)
    scale = logit_scale / sums
    scale_column = scale.reshape(samples, 1)
    at_target = jnp.where(ids >= 0, scale * patch, 0.0).reshape(samples, 1)
    pull = (pull * scale_column + at_target * goal.astype(f32)).astype(bf16)
    scaled = (emb_low.astype(f32) * scale_column).astype(bf16)
    parcel = jnp.concatenate([pull.reshape(chips, own, depth), cargo], axis=2)
    parcel = to_chips(parcel)

    other_push = pushed(ids, patch, scaled, exps, 1)
    other_push = swapped(other_push)
    grad_centers = pushed(ids, patch, scaled, exps, 0, centers, other_push)

    own_float = embedded.astype(f32)
    inv_emb = inverse_norm(own_float, 1)
    emb_dir = own_float * inv_emb
    grad_dir = jnp.sum(parcel[:, :, :depth].astype(f32), axis=0)
    grad_emb = (
        (grad_dir - emb_dir * jnp.sum(grad_dir * emb_dir, axis=1, keepdims=True)) * inv_emb
    ).astype(bf16)
    grads = from_chips(grad_emb).reshape(samples, depth)

    columns = parcel[:, :, depth:].reshape(samples, 256)
    both = lax.dot_general(columns, grads, (((0,), (0,)), ((), ())), preferred_element_type=f32)
    theirs_fc = swapped(both[128 : 128 + fcols])
    grad_fc = both[:fcols] + theirs_fc
    own_sums = lax.dynamic_slice_in_dim(sums.reshape(samples), chip * own, own)
    loss = jnp.log(own_sums) - report[0, samples : samples + own]
    return (loss, grad_centers, grad_fc)


def solution(mesh):
    torus = Mesh(mesh.devices.reshape(4, 4, 4, 2), CLS)
    placed = (P(CLS, None), P(), P(CLS, None), P())
    return jax.shard_map(
        step,
        mesh=torus,
        in_specs=placed,
        out_specs=(P(CLS), P(CLS, None), P(CLS, None)),
        check_vma=False,
    )
```

```python
import functools
import math

import jax
import jax.numpy as jnp
from jax import lax
from jax.experimental import pallas as pl
from jax.experimental.pallas import tpu as pltpu
from jax.sharding import Mesh
from jax.sharding import PartitionSpec as P


CLS = ("cls_0", "cls_1", "cls_2", "cls_3")
CHIP = ("cls_0", "cls_1", "cls_2")
CORE = "cls_3"

logit_scale = 64.0
cos_margin = math.cos(0.5)
sin_margin = math.sin(0.5)
epsilon = 1e-06

f32 = jnp.float32
bf16 = jnp.bfloat16


def swapped(x):
    return lax.ppermute(x, CORE, [(0, 1), (1, 0)])


def to_chips(x):
    return lax.all_to_all(x, CHIP, split_axis=0, concat_axis=0, tiled=True)


def from_chips(x):
    copies = jnp.broadcast_to(x, (lax.axis_size(CHIP), *x.shape))
    return lax.all_to_all(copies, CHIP, split_axis=0, concat_axis=0, tiled=True)


def inverse_norm(values, axis):
    return lax.rsqrt(jnp.sum(values * values, axis=axis, keepdims=True) + epsilon)


def margin(target_cos):
    target_sine = jnp.sqrt(1.0 - target_cos * target_cos)
    margined = target_cos * cos_margin - target_sine * sin_margin
    slope = cos_margin + sin_margin * target_cos / target_sine
    return margined, slope


ANY = pl.BlockSpec(memory_space=pl.ANY)
VMEM = pl.BlockSpec(memory_space=pltpu.VMEM)
SMEM = pl.BlockSpec(memory_space=pltpu.SMEM)


def embed_kernel(cuts, f_ref, w_ref, out_ref, copies_ref, weight, sems):
    copies = [
        pltpu.make_async_copy(w_ref.at[pl.ds(a, b - a)], weight.at[pl.ds(a, b - a)], sems.at[k])
        for k, (a, b) in enumerate(zip(cuts, cuts[1:]))
    ]
    for copy in copies:
        copy.start()
    total = None
    for copy, a, b in zip(copies, cuts, cuts[1:]):
        copy.wait()
        product = jnp.dot(f_ref[:, a:b], weight[a:b, :], preferred_element_type=f32)
        total = product if total is None else total + product
    rows = total.astype(bf16)
    out_ref[...] = rows
    for chip in range(copies_ref.shape[0]):
        copies_ref[chip] = rows


def embedded_rows(features, weight, chips, cuts):
    own, wide = features.shape
    depth = weight.shape[1]
    return pl.pallas_call(
        functools.partial(embed_kernel, cuts),
        in_specs=[VMEM, ANY],
        out_specs=[VMEM, VMEM],
        out_shape=[
            jax.ShapeDtypeStruct((own, depth), bf16),
            jax.ShapeDtypeStruct((chips, own, depth), bf16),
        ],
        scratch_shapes=[pltpu.VMEM((wide, depth), bf16), pltpu.SemaphoreType.DMA((len(cuts) - 1,))],
        cost_estimate=pl.CostEstimate(
            flops=2 * own * wide * depth, bytes_accessed=2 * wide * depth, transcendentals=0
        ),
        name="embed",
    )(features, weight)


def targets_kernel(batch, ids_ref, busy_ref, own_ref, other_ref, goal_ref, centers, found, sems):
    count, depth = own_ref.shape
    copies = [
        pltpu.make_async_copy(part, centers.at[pl.ds(k * count, count)], sems.at[k])
        for k, part in enumerate((own_ref, other_ref))
    ]
    for copy in copies:
        copy.start()
    found[...] = jnp.zeros_like(found)
    for copy in copies:
        copy.wait()
    spot = lax.broadcasted_iota(jnp.int32, (16, depth), 0)

    def group(g, carry):
        @pl.when(busy_ref[g] >= 0)
        def _():
            def sample(b, carry):
                at = g * batch + b
                row = ids_ref[0, at]

                @pl.when(row >= 0)
                def _():
                    near = centers[pl.ds(pl.multiple_of(row // 16 * 16, 16), 16), :].astype(f32)
                    found[pl.ds(at, 1), :] = jnp.sum(jnp.where(spot == row % 16, near, 0.0), axis=0, keepdims=True)

                return carry

            lax.fori_loop(0, batch, sample, 0)

        return carry

    lax.fori_loop(0, busy_ref.shape[0], group, 0)
    rows = found[...]
    goal_ref[...] = (rows * inverse_norm(rows, 1)).astype(bf16)


def target_directions(ids, batch, own, other):
    count, depth = own.shape
    samples = ids.shape[1]
    busy = jnp.max(ids.reshape(samples // batch, batch), axis=1)
    return pl.pallas_call(
        functools.partial(targets_kernel, batch),
        in_specs=[SMEM, SMEM, ANY, ANY],
        out_specs=VMEM,
        out_shape=jax.ShapeDtypeStruct((samples, depth), bf16),
        scratch_shapes=[
            pltpu.VMEM((2 * count, depth), bf16),
            pltpu.VMEM((samples, depth), f32),
            pltpu.SemaphoreType.DMA((2,)),
        ],
        cost_estimate=pl.CostEstimate(
            flops=2 * count * depth * samples, bytes_accessed=4 * count * depth, transcendentals=0
        ),
        name="targets",
    )(ids, busy, own, other)


def row_of(values):
    part = values[:, :128]
    for k in range(1, values.shape[1] // 128):
        part = part + values[:, k * 128 : (k + 1) * 128]
    return jnp.sum(part.T, axis=0, keepdims=True)


def exp_kernel(steps, early, lanes, ids_ref, x_ref, goal_ref, own_ref, other_ref, exp_ref, low_ref, pull_ref, emb_ref,
               report_ref, cos_ref, wide_ids, scaled, row_sum, total):
    i = pl.program_id(0)
    rows = own_ref.shape[0]
    samples = x_ref.shape[0]
    sub = samples // lanes

    @pl.when(i == 0)
    def _():
        wide_ids[...] = jnp.broadcast_to(ids_ref[...], (128, samples)).T
        x = x_ref[...].astype(f32)
        emb = (x * inverse_norm(x, 1)).astype(bf16)
        emb_ref[...] = emb
        scaled[...] = (emb * logit_scale).astype(bf16)
        row_sum[...] = jnp.zeros_like(row_sum)
        total[...] = jnp.zeros_like(total)

    def chunk(with_pull):
        block = jnp.where(i < steps, own_ref[...], other_ref[...]).astype(f32)
        low_ref[...] = (block * inverse_norm(block, 1)).astype(bf16)
        columns = lax.broadcasted_iota(jnp.int32, (sub, 128), 1)

        def products(m):
            return lax.dot_general(
                scaled[m * sub : (m + 1) * sub, :],
                low_ref[...],
                (((1,), (1,)), ((), ())),
                preferred_element_type=f32,
            )

        logits = products(0)
        for m in range(lanes):
            later = products(m + 1) if m + 1 < lanes else None
            span = slice(m * sub, (m + 1) * sub)
            ids = wide_ids[span, :] - i * rows
            part = None
            for t in range(rows // 128):
                weight = jnp.exp(logits[:, t * 128 : (t + 1) * 128])
                weight = jnp.where(columns + t * 128 == ids, 0.0, weight)
                part = weight if part is None else part + weight
                exp_ref[span, t * 128 : (t + 1) * 128] = weight.astype(bf16)
            row_sum[span, :] += part
            if with_pull:
                total[span, :] += jnp.dot(exp_ref[span, :], low_ref[...], preferred_element_type=f32)
            logits = later

    @pl.when(i < early)
    def _():
        chunk(True)

    @pl.when(i >= early)
    def _():
        chunk(False)

    @pl.when(i == early)
    def _():
        pull_ref[...] = total[...]

    @pl.when(i == 2 * steps - 1)
    def _():
        target_cos = row_of(goal_ref[...].astype(f32) * scaled[...].astype(f32)) * (1.0 / logit_scale)
        cos_ref[...] = target_cos
        margined, _ = margin(target_cos)
        is_here = ids_ref[...] >= 0
        logit = jnp.where(is_here, logit_scale * margined, 0.0)
        sums = row_of(row_sum[...]) + jnp.where(is_here, jnp.exp(logit_scale * margined), 0.0)
        chips = report_ref.shape[0]
        own = samples // chips
        lane = lax.broadcasted_iota(jnp.int32, (1, 128), 1)
        for chip in range(chips):
            k = chip * own // 128
            theirs = (lane + k * 128) // own == chip
            report_ref[chip, :, :samples] = sums
            report_ref[chip, :, samples:] = jnp.where(theirs, logit[:, k * 128 : (k + 1) * 128], 0.0)


def exponentials(ids, x, goal, own, other, chips, early, rows=1024, lanes=2):
    samples, depth = x.shape
    count = own.shape[0]
    steps = count // rows
    late = 2 * steps - early
    fixed = lambda i: (0, 0)
    return pl.pallas_call(
        functools.partial(exp_kernel, steps, early, lanes),
        grid=(2 * steps,),
        in_specs=[
            pl.BlockSpec((1, samples), fixed),
            pl.BlockSpec((samples, depth), fixed),
            pl.BlockSpec((samples, depth), fixed),
            pl.BlockSpec((rows, depth), lambda i: (jnp.minimum(i, steps - 1), 0)),
            pl.BlockSpec((rows, depth), lambda i: (jnp.maximum(i - steps, 0), 0)),
        ],
        out_specs=[
            pl.BlockSpec((samples, rows), lambda i: (0, i)),
            pl.BlockSpec((rows, depth), lambda i: (jnp.maximum(i - early, 0), 0)),
            pl.BlockSpec((samples, depth), fixed),
            pl.BlockSpec((samples, depth), fixed),
            pl.BlockSpec((chips, 1, samples + 128), lambda i: (0, 0, 0)),
            pl.BlockSpec((1, samples), fixed),
        ],
        out_shape=[
            jax.ShapeDtypeStruct((samples, 2 * count), bf16),
            jax.ShapeDtypeStruct((late * rows, depth), bf16),
            jax.ShapeDtypeStruct((samples, depth), f32),
            jax.ShapeDtypeStruct((samples, depth), bf16),
            jax.ShapeDtypeStruct((chips, 1, samples + 128), f32),
            jax.ShapeDtypeStruct((1, samples), f32),
        ],
        scratch_shapes=[
            pltpu.VMEM((samples, 128), jnp.int32),
            pltpu.VMEM((samples, depth), bf16),
            pltpu.VMEM((samples, 128), f32),
            pltpu.VMEM((samples, depth), f32),
        ],
        cost_estimate=pl.CostEstimate(
            flops=4 * count * depth * samples,
            bytes_accessed=8 * count * depth,
            transcendentals=2 * count * samples,
        ),
        name="exponentials",
    )(ids, x, goal, own, other)


def pull_kernel(early, rows, exp_ref, low_ref, start_ref, out_ref, exps, lows, exp_sems, low_sems, start_sem):
    steps = low_ref.shape[0] // rows
    start = pltpu.make_async_copy(start_ref, out_ref, start_sem)

    def fetch(i, slot):
        return (
            pltpu.make_async_copy(
                exp_ref.at[:, pl.ds((early + i) * rows, rows)], exps.at[slot], exp_sems.at[slot]
            ),
            pltpu.make_async_copy(low_ref.at[pl.ds(i * rows, rows)], lows.at[slot], low_sems.at[slot]),
        )

    for i in range(steps):
        for copy in fetch(i, i):
            copy.start()
        if i == 0:
            start.start()
    for i in range(steps):
        for copy in fetch(i, i):
            copy.wait()
        if i == 0:
            start.wait()
        out_ref[...] += jnp.dot(exps[i], lows[i], preferred_element_type=f32)


def pulled(exps, low, start, early, rows=1024):
    samples = exps.shape[0]
    count, depth = low.shape
    steps = count // rows
    return pl.pallas_call(
        functools.partial(pull_kernel, early, rows),
        in_specs=[ANY, ANY, ANY],
        out_specs=VMEM,
        out_shape=jax.ShapeDtypeStruct((samples, depth), f32),
        scratch_shapes=[
            pltpu.VMEM((steps, samples, rows), bf16),
            pltpu.VMEM((steps, rows, depth), bf16),
            pltpu.SemaphoreType.DMA((steps,)),
            pltpu.SemaphoreType.DMA((steps,)),
            pltpu.SemaphoreType.DMA,
        ],
        cost_estimate=pl.CostEstimate(
            flops=2 * count * depth * samples, bytes_accessed=2 * count * (depth + samples), transcendentals=0
        ),
        name="pull",
    )(exps, low, start)


def settle_kernel(ids_ref, cos_ref, report_ref, pull_ref, goal_ref, emb_ref, cargo_ref, parcel_ref, scaled_ref,
                  patch_ref, sums_ref, wide_scale, wide_target):
    i = pl.program_id(0)
    rows, depth = goal_ref.shape
    samples = ids_ref.shape[1]

    @pl.when(i == 0)
    def _():
        report = jnp.sum(report_ref[...], axis=0)
        sums_ref[...] = report
        sums = report[:, :samples]
        margined, slope = margin(cos_ref[...])
        patch = slope * (jnp.exp(logit_scale * margined) - sums)
        patch_ref[...] = patch
        scale = logit_scale / sums
        at_target = jnp.where(ids_ref[...] >= 0, scale * patch, 0.0)
        wide_scale[...] = jnp.broadcast_to(scale, (128, samples)).T
        wide_target[...] = jnp.broadcast_to(at_target, (128, samples)).T

    span = pl.ds(pl.multiple_of(i * rows, rows), rows)
    scale = jnp.concatenate([wide_scale[span, :]] * (depth // 128), axis=1)
    at_target = jnp.concatenate([wide_target[span, :]] * (depth // 128), axis=1)
    parcel_ref[:, :depth] = (pull_ref[...] * scale + at_target * goal_ref[...].astype(f32)).astype(bf16)
    parcel_ref[:, depth:] = cargo_ref[...]
    scaled_ref[...] = (emb_ref[...].astype(f32) * scale).astype(bf16)


def settled(ids, target_cos, report, pull, goal, emb, cargo, rows=512):
    samples, depth = emb.shape
    extra = cargo.shape[1]
    fixed = lambda i: (0, 0)
    step = lambda i: (i, 0)
    row = pl.BlockSpec((1, samples), fixed)
    return pl.pallas_call(
        settle_kernel,
        grid=(samples // rows,),
        in_specs=[row, row, pl.BlockSpec(report.shape, lambda i: (0, 0, 0))]
        + [pl.BlockSpec((rows, depth), step)] * 3
        + [pl.BlockSpec((rows, extra), step)],
        out_specs=[
            pl.BlockSpec((rows, depth + extra), step),
            pl.BlockSpec((rows, depth), step),
            row,
            pl.BlockSpec((1, report.shape[2]), fixed),
        ],
        out_shape=[
            jax.ShapeDtypeStruct((samples, depth + extra), bf16),
            jax.ShapeDtypeStruct((samples, depth), bf16),
            jax.ShapeDtypeStruct((1, samples), f32),
            jax.ShapeDtypeStruct((1, report.shape[2]), f32),
        ],
        scratch_shapes=[pltpu.VMEM((samples, 128), f32), pltpu.VMEM((samples, 128), f32)],
        cost_estimate=pl.CostEstimate(
            flops=8 * samples * depth, bytes_accessed=14 * samples * depth, transcendentals=0
        ),
        name="settle",
    )(ids, target_cos, report, pull, goal, emb, cargo)


def push_kernel(base, final, ids_ref, patch_ref, emb_ref, exp_ref, *refs):
    i = pl.program_id(0)
    samples, rows = exp_ref.shape
    if final:
        c_ref, other_ref, out_ref, wide_ids, wide_patch = refs
    else:
        out_ref, wide_ids, wide_patch = refs

    @pl.when(i == 0)
    def _():
        wide_ids[...] = jnp.broadcast_to(ids_ref[...], (128, samples)).T
        wide_patch[...] = jnp.broadcast_to(patch_ref[...], (128, samples)).T

    ids = jnp.concatenate([wide_ids[...] - (base + i) * rows] * (rows // 128), axis=1)
    patch = jnp.concatenate([wide_patch[...]] * (rows // 128), axis=1)
    hit = lax.broadcasted_iota(jnp.int32, exp_ref.shape, 1) == ids
    weight = jnp.where(hit, patch, exp_ref[...].astype(f32)).astype(bf16)
    push = lax.dot_general(weight, emb_ref[...], (((0,), (0,)), ((), ())), preferred_element_type=f32)
    if final:
        push = push + other_ref[...].astype(f32)
        block = c_ref[...].astype(f32)
        inv = inverse_norm(block, 1)
        unit = block * inv
        push = (push - unit * jnp.sum(push * unit, axis=1, keepdims=True)) * inv
    out_ref[...] = push.astype(bf16)


def pushed(ids, patch, emb, exps, half, centers=None, other=None, rows=1024):
    samples, depth = emb.shape
    count = exps.shape[1] // 2
    base = half * (count // rows)
    final = centers is not None
    fixed = lambda i: (0, 0)
    step = lambda i: (i, 0)
    extra = (centers, other) if final else ()
    return pl.pallas_call(
        functools.partial(push_kernel, base, final),
        grid=(count // rows,),
        in_specs=[
            pl.BlockSpec((1, samples), fixed),
            pl.BlockSpec((1, samples), fixed),
            pl.BlockSpec((samples, depth), fixed),
            pl.BlockSpec((samples, rows), lambda i: (0, base + i)),
        ]
        + [pl.BlockSpec((rows, depth), step)] * len(extra),
        out_specs=pl.BlockSpec((rows, depth), step),
        out_shape=jax.ShapeDtypeStruct((count, depth), bf16),
        scratch_shapes=[pltpu.VMEM((samples, 128), jnp.int32), pltpu.VMEM((samples, 128), f32)],
        cost_estimate=pl.CostEstimate(
            flops=2 * count * depth * samples, bytes_accessed=2 * count * samples, transcendentals=0
        ),
    )(ids, patch, emb, exps, *extra)


def step(features, fc_weight, centers, labels):
    own, wide = features.shape
    class_rows, depth = centers.shape
    chips = lax.axis_size(CHIP)
    chip = lax.axis_index(CHIP)
    core = lax.axis_index(CORE)
    samples = chips * own

    other_centers = swapped(centers)
    cuts = tuple(range(0, wide, 1792)) + (wide,)
    embedded, copies = embedded_rows(features, fc_weight, chips, cuts)
    x = to_chips(copies).reshape(samples, depth)

    by_core = labels.reshape(chips, 2, own)
    my_labels = jnp.where(core == 0, by_core[:, 0], by_core[:, 1]).reshape(1, samples)
    local = my_labels - chip * (2 * class_rows)
    inside = (local >= 0) & (local < 2 * class_rows)
    turned_ids = jnp.where(core == 0, local, (local + class_rows) % (2 * class_rows))
    ids = jnp.where(inside, turned_ids, -1)

    split = features.reshape(own, chips, 2, wide // (2 * chips))
    mine = jnp.where(core == 0, split[:, :, 0], split[:, :, 1])
    theirs = jnp.where(core == 0, split[:, :, 1], split[:, :, 0])
    fcols = mine.shape[-1]
    pad = ((0, 0), (0, 0), (0, 128 - fcols))
    cargo = jnp.concatenate([jnp.pad(mine.swapaxes(0, 1), pad), jnp.pad(theirs.swapaxes(0, 1), pad)], axis=2)

    goal = target_directions(ids, own, centers, other_centers)
    early = 6
    exps, low, pull, emb_low, report, target_cos = exponentials(ids, x, goal, centers, other_centers, chips, early)
    report = to_chips(report)
    pull = pulled(exps, low, pull, early)
    parcel, scaled, patch, report = settled(
        ids, target_cos, report, pull, goal, emb_low, cargo.reshape(samples, 256)
    )
    parcel = to_chips(parcel.reshape(chips, own, depth + 256))

    other_push = pushed(ids, patch, scaled, exps, 1)
    other_push = swapped(other_push)
    grad_centers = pushed(ids, patch, scaled, exps, 0, centers, other_push)

    own_float = embedded.astype(f32)
    inv_emb = inverse_norm(own_float, 1)
    emb_dir = own_float * inv_emb
    grad_dir = jnp.sum(parcel[:, :, :depth].astype(f32), axis=0)
    grad_emb = (
        (grad_dir - emb_dir * jnp.sum(grad_dir * emb_dir, axis=1, keepdims=True)) * inv_emb
    ).astype(bf16)
    grads = from_chips(grad_emb).reshape(samples, depth)

    columns = parcel[:, :, depth:].reshape(samples, 256)
    both = lax.dot_general(columns, grads, (((0,), (0,)), ((), ())), preferred_element_type=f32)
    theirs_fc = swapped(both[128 : 128 + fcols])
    grad_fc = both[:fcols] + theirs_fc
    own_sums = lax.dynamic_slice_in_dim(report[0], chip * own, own)
    own_logits = lax.dynamic_slice_in_dim(report[0], samples + chip * own % 128, own)
    loss = jnp.log(own_sums) - own_logits
    return (loss, grad_centers, grad_fc)


def solution(mesh):
    torus = Mesh(mesh.devices.reshape(4, 4, 4, 2), CLS)
    placed = (P(CLS, None), P(), P(CLS, None), P())
    return jax.shard_map(
        step,
        mesh=torus,
        in_specs=placed,
        out_specs=(P(CLS), P(CLS, None), P(CLS, None)),
        check_vma=False,
    )
```

```python
import functools
import math

import jax
import jax.numpy as jnp
from jax import lax
from jax.experimental import pallas as pl
from jax.experimental.pallas import tpu as pltpu
from jax.sharding import Mesh
from jax.sharding import PartitionSpec as P


CLS = ("cls_0", "cls_1", "cls_2", "cls_3")
CHIP = ("cls_0", "cls_1", "cls_2")
CORE = "cls_3"

logit_scale = 64.0
cos_margin = math.cos(0.5)
sin_margin = math.sin(0.5)
epsilon = 1e-06

f32 = jnp.float32
bf16 = jnp.bfloat16


def swapped(x):
    return lax.ppermute(x, CORE, [(0, 1), (1, 0)])


def to_chips(x):
    return lax.all_to_all(x, CHIP, split_axis=0, concat_axis=0, tiled=True)


def from_chips(x):
    copies = jnp.broadcast_to(x, (lax.axis_size(CHIP), *x.shape))
    return lax.all_to_all(copies, CHIP, split_axis=0, concat_axis=0, tiled=True)


def inverse_norm(values, axis):
    return lax.rsqrt(jnp.sum(values * values, axis=axis, keepdims=True) + epsilon)


def margin(target_cos):
    target_sine = jnp.sqrt(1.0 - target_cos * target_cos)
    margined = target_cos * cos_margin - target_sine * sin_margin
    slope = cos_margin + sin_margin * target_cos / target_sine
    return margined, slope


ANY = pl.BlockSpec(memory_space=pl.ANY)
VMEM = pl.BlockSpec(memory_space=pltpu.VMEM)
SMEM = pl.BlockSpec(memory_space=pltpu.SMEM)


def embed_kernel(cuts, core_ref, f_ref, w_ref, out_ref, parcel_ref, weight, sems):
    copies = [
        pltpu.make_async_copy(w_ref.at[pl.ds(a, b - a)], weight.at[pl.ds(a, b - a)], sems.at[k])
        for k, (a, b) in enumerate(zip(cuts, cuts[1:]))
    ]
    for copy in copies:
        copy.start()
    chips = parcel_ref.shape[0]
    own, wide = f_ref.shape
    depth = out_ref.shape[1]
    fcols = wide // (2 * chips)
    lower = core_ref[0] == 0
    pad = jnp.zeros((own, 128 - fcols), bf16)
    for chip in range(chips):
        at = 2 * chip * fcols
        first = jnp.concatenate([f_ref[:, at : at + fcols], pad], axis=1)
        second = jnp.concatenate([f_ref[:, at + fcols : at + 2 * fcols], pad], axis=1)
        parcel_ref[chip, :, depth : depth + 128] = jnp.where(lower, first, second)
        parcel_ref[chip, :, depth + 128 :] = jnp.where(lower, second, first)
    total = None
    for copy, a, b in zip(copies, cuts, cuts[1:]):
        copy.wait()
        product = jnp.dot(f_ref[:, a:b], weight[a:b, :], preferred_element_type=f32)
        total = product if total is None else total + product
    rows = total.astype(bf16)
    out_ref[...] = rows
    for chip in range(chips):
        parcel_ref[chip, :, :depth] = rows


def embedded_rows(core, features, weight, chips, cuts):
    own, wide = features.shape
    depth = weight.shape[1]
    return pl.pallas_call(
        functools.partial(embed_kernel, cuts),
        in_specs=[SMEM, VMEM, ANY],
        out_specs=[VMEM, VMEM],
        out_shape=[
            jax.ShapeDtypeStruct((own, depth), bf16),
            jax.ShapeDtypeStruct((chips, own, depth + 256), bf16),
        ],
        scratch_shapes=[pltpu.VMEM((wide, depth), bf16), pltpu.SemaphoreType.DMA((len(cuts) - 1,))],
        cost_estimate=pl.CostEstimate(
            flops=2 * own * wide * depth, bytes_accessed=2 * wide * depth, transcendentals=0
        ),
        name="embed",
    )(core, features, weight)


def targets_kernel(batch, ids_ref, busy_ref, own_ref, other_ref, goal_ref, centers, found, sems):
    count, depth = own_ref.shape
    copies = [
        pltpu.make_async_copy(part, centers.at[pl.ds(k * count, count)], sems.at[k])
        for k, part in enumerate((own_ref, other_ref))
    ]
    for copy in copies:
        copy.start()
    found[...] = jnp.zeros_like(found)
    for copy in copies:
        copy.wait()
    spot = lax.broadcasted_iota(jnp.int32, (16, depth), 0)

    def group(g, carry):
        @pl.when(busy_ref[g] >= 0)
        def _():
            def sample(b, carry):
                at = g * batch + b
                row = ids_ref[0, at]

                @pl.when(row >= 0)
                def _():
                    near = centers[pl.ds(pl.multiple_of(row // 16 * 16, 16), 16), :].astype(f32)
                    found[pl.ds(at, 1), :] = jnp.sum(jnp.where(spot == row % 16, near, 0.0), axis=0, keepdims=True)

                return carry

            lax.fori_loop(0, batch, sample, 0)

        return carry

    lax.fori_loop(0, busy_ref.shape[0], group, 0)
    rows = found[...]
    goal_ref[...] = (rows * inverse_norm(rows, 1)).astype(bf16)


def target_directions(ids, batch, own, other):
    count, depth = own.shape
    samples = ids.shape[1]
    busy = jnp.max(ids.reshape(samples // batch, batch), axis=1)
    return pl.pallas_call(
        functools.partial(targets_kernel, batch),
        in_specs=[SMEM, SMEM, ANY, ANY],
        out_specs=VMEM,
        out_shape=jax.ShapeDtypeStruct((samples, depth), bf16),
        scratch_shapes=[
            pltpu.VMEM((2 * count, depth), bf16),
            pltpu.VMEM((samples, depth), f32),
            pltpu.SemaphoreType.DMA((2,)),
        ],
        cost_estimate=pl.CostEstimate(
            flops=2 * count * depth * samples, bytes_accessed=4 * count * depth, transcendentals=0
        ),
        name="targets",
    )(ids, busy, own, other)


def row_of(values):
    part = values[:, :128]
    for k in range(1, values.shape[1] // 128):
        part = part + values[:, k * 128 : (k + 1) * 128]
    return jnp.sum(part.T, axis=0, keepdims=True)


def exp_kernel(steps, early, lanes, ids_ref, x_ref, goal_ref, own_ref, other_ref, exp_ref, low_ref, pull_ref, emb_ref,
               report_ref, cos_ref, wide_ids, scaled, row_sum, total):
    i = pl.program_id(0)
    rows = own_ref.shape[0]
    samples = x_ref.shape[0]
    sub = samples // lanes

    @pl.when(i == 0)
    def _():
        wide_ids[...] = jnp.broadcast_to(ids_ref[...], (128, samples)).T
        x = x_ref[...].astype(f32)
        emb = (x * inverse_norm(x, 1)).astype(bf16)
        emb_ref[...] = emb
        scaled[...] = (emb * logit_scale).astype(bf16)
        row_sum[...] = jnp.zeros_like(row_sum)
        total[...] = jnp.zeros_like(total)

    def chunk(with_pull):
        block = jnp.where(i < steps, own_ref[...], other_ref[...]).astype(f32)
        low_ref[...] = (block * inverse_norm(block, 1)).astype(bf16)
        columns = lax.broadcasted_iota(jnp.int32, (sub, 128), 1)

        def products(m):
            return lax.dot_general(
                scaled[m * sub : (m + 1) * sub, :],
                low_ref[...],
                (((1,), (1,)), ((), ())),
                preferred_element_type=f32,
            )

        logits = products(0)
        for m in range(lanes):
            later = products(m + 1) if m + 1 < lanes else None
            span = slice(m * sub, (m + 1) * sub)
            ids = wide_ids[span, :] - i * rows
            part = None
            for t in range(rows // 128):
                weight = jnp.exp(logits[:, t * 128 : (t + 1) * 128])
                weight = jnp.where(columns + t * 128 == ids, 0.0, weight)
                part = weight if part is None else part + weight
                exp_ref[span, t * 128 : (t + 1) * 128] = weight.astype(bf16)
            row_sum[span, :] += part
            if with_pull:
                total[span, :] += jnp.dot(exp_ref[span, :], low_ref[...], preferred_element_type=f32)
            logits = later

    @pl.when(i < early)
    def _():
        chunk(True)

    @pl.when(i >= early)
    def _():
        chunk(False)

    @pl.when(i == early)
    def _():
        pull_ref[...] = total[...]

    @pl.when(i == 2 * steps - 1)
    def _():
        target_cos = row_of(goal_ref[...].astype(f32) * scaled[...].astype(f32)) * (1.0 / logit_scale)
        cos_ref[...] = target_cos
        margined, _ = margin(target_cos)
        is_here = ids_ref[...] >= 0
        logit = jnp.where(is_here, logit_scale * margined, 0.0)
        sums = row_of(row_sum[...]) + jnp.where(is_here, jnp.exp(logit_scale * margined), 0.0)
        chips = report_ref.shape[0]
        own = samples // chips
        lane = lax.broadcasted_iota(jnp.int32, (1, 128), 1)
        for chip in range(chips):
            k = chip * own // 128
            theirs = (lane + k * 128) // own == chip
            report_ref[chip, :, :samples] = sums
            report_ref[chip, :, samples:] = jnp.where(theirs, logit[:, k * 128 : (k + 1) * 128], 0.0)


def exponentials(ids, x, goal, own, other, chips, early, rows=1024, lanes=2):
    samples = x.shape[0]
    count, depth = own.shape
    steps = count // rows
    late = 2 * steps - early
    fixed = lambda i: (0, 0)
    return pl.pallas_call(
        functools.partial(exp_kernel, steps, early, lanes),
        grid=(2 * steps,),
        in_specs=[
            pl.BlockSpec((1, samples), fixed),
            pl.BlockSpec((samples, depth), fixed),
            pl.BlockSpec((samples, depth), fixed),
            pl.BlockSpec((rows, depth), lambda i: (jnp.minimum(i, steps - 1), 0)),
            pl.BlockSpec((rows, depth), lambda i: (jnp.maximum(i - steps, 0), 0)),
        ],
        out_specs=[
            pl.BlockSpec((samples, rows), lambda i: (0, i)),
            pl.BlockSpec((rows, depth), lambda i: (jnp.maximum(i - early, 0), 0)),
            pl.BlockSpec((samples, depth), fixed),
            pl.BlockSpec((samples, depth), fixed),
            pl.BlockSpec((chips, 1, samples + 128), lambda i: (0, 0, 0)),
            pl.BlockSpec((1, samples), fixed),
        ],
        out_shape=[
            jax.ShapeDtypeStruct((samples, 2 * count), bf16),
            jax.ShapeDtypeStruct((late * rows, depth), bf16),
            jax.ShapeDtypeStruct((samples, depth), f32),
            jax.ShapeDtypeStruct((samples, depth), bf16),
            jax.ShapeDtypeStruct((chips, 1, samples + 128), f32),
            jax.ShapeDtypeStruct((1, samples), f32),
        ],
        scratch_shapes=[
            pltpu.VMEM((samples, 128), jnp.int32),
            pltpu.VMEM((samples, depth), bf16),
            pltpu.VMEM((samples, 128), f32),
            pltpu.VMEM((samples, depth), f32),
        ],
        cost_estimate=pl.CostEstimate(
            flops=4 * count * depth * samples,
            bytes_accessed=8 * count * depth,
            transcendentals=2 * count * samples,
        ),
        name="exponentials",
    )(ids, x, goal, own, other)


def pull_kernel(early, rows, exp_ref, low_ref, start_ref, out_ref, exps, lows, exp_sems, low_sems, start_sem):
    steps = low_ref.shape[0] // rows
    start = pltpu.make_async_copy(start_ref, out_ref, start_sem)

    def fetch(i, slot):
        return (
            pltpu.make_async_copy(
                exp_ref.at[:, pl.ds((early + i) * rows, rows)], exps.at[slot], exp_sems.at[slot]
            ),
            pltpu.make_async_copy(low_ref.at[pl.ds(i * rows, rows)], lows.at[slot], low_sems.at[slot]),
        )

    for i in range(steps):
        for copy in fetch(i, i):
            copy.start()
        if i == 0:
            start.start()
    for i in range(steps):
        for copy in fetch(i, i):
            copy.wait()
        if i == 0:
            start.wait()
        out_ref[...] += jnp.dot(exps[i], lows[i], preferred_element_type=f32)


def pulled(exps, low, start, early, rows=1024):
    samples = exps.shape[0]
    count, depth = low.shape
    steps = count // rows
    return pl.pallas_call(
        functools.partial(pull_kernel, early, rows),
        in_specs=[ANY, ANY, ANY],
        out_specs=VMEM,
        out_shape=jax.ShapeDtypeStruct((samples, depth), f32),
        scratch_shapes=[
            pltpu.VMEM((steps, samples, rows), bf16),
            pltpu.VMEM((steps, rows, depth), bf16),
            pltpu.SemaphoreType.DMA((steps,)),
            pltpu.SemaphoreType.DMA((steps,)),
            pltpu.SemaphoreType.DMA,
        ],
        cost_estimate=pl.CostEstimate(
            flops=2 * count * depth * samples, bytes_accessed=2 * count * (depth + samples), transcendentals=0
        ),
        name="pull",
    )(exps, low, start)


def settle_kernel(ids_ref, cos_ref, report_ref, pull_ref, goal_ref, emb_ref, parcel_ref, scaled_ref,
                  patch_ref, sums_ref, wide_scale, wide_target):
    i = pl.program_id(0)
    rows, depth = goal_ref.shape
    samples = ids_ref.shape[1]

    @pl.when(i == 0)
    def _():
        report = jnp.sum(report_ref[...], axis=0)
        sums_ref[...] = report
        sums = report[:, :samples]
        margined, slope = margin(cos_ref[...])
        patch = slope * (jnp.exp(logit_scale * margined) - sums)
        patch_ref[...] = patch
        scale = logit_scale / sums
        at_target = jnp.where(ids_ref[...] >= 0, scale * patch, 0.0)
        wide_scale[...] = jnp.broadcast_to(scale, (128, samples)).T
        wide_target[...] = jnp.broadcast_to(at_target, (128, samples)).T

    span = pl.ds(pl.multiple_of(i * rows, rows), rows)
    scale = jnp.concatenate([wide_scale[span, :]] * (depth // 128), axis=1)
    at_target = jnp.concatenate([wide_target[span, :]] * (depth // 128), axis=1)
    parcel_ref[...] = (pull_ref[...] * scale + at_target * goal_ref[...].astype(f32)).astype(bf16)
    scaled_ref[...] = (emb_ref[...].astype(f32) * scale).astype(bf16)


def settled(ids, target_cos, report, pull, goal, emb, rows=512):
    samples, depth = emb.shape
    fixed = lambda i: (0, 0)
    step = lambda i: (i, 0)
    row = pl.BlockSpec((1, samples), fixed)
    return pl.pallas_call(
        settle_kernel,
        grid=(samples // rows,),
        in_specs=[row, row, pl.BlockSpec(report.shape, lambda i: (0, 0, 0))]
        + [pl.BlockSpec((rows, depth), step)] * 3,
        out_specs=[
            pl.BlockSpec((rows, depth), step),
            pl.BlockSpec((rows, depth), step),
            row,
            pl.BlockSpec((1, report.shape[2]), fixed),
        ],
        out_shape=[
            jax.ShapeDtypeStruct((samples, depth), bf16),
            jax.ShapeDtypeStruct((samples, depth), bf16),
            jax.ShapeDtypeStruct((1, samples), f32),
            jax.ShapeDtypeStruct((1, report.shape[2]), f32),
        ],
        scratch_shapes=[pltpu.VMEM((samples, 128), f32), pltpu.VMEM((samples, 128), f32)],
        cost_estimate=pl.CostEstimate(
            flops=8 * samples * depth, bytes_accessed=14 * samples * depth, transcendentals=0
        ),
        name="settle",
    )(ids, target_cos, report, pull, goal, emb)


def push_kernel(base, final, ids_ref, patch_ref, emb_ref, exp_ref, *refs):
    i = pl.program_id(0)
    samples, rows = exp_ref.shape
    if final:
        c_ref, other_ref, out_ref, wide_ids, wide_patch = refs
    else:
        out_ref, wide_ids, wide_patch = refs

    @pl.when(i == 0)
    def _():
        wide_ids[...] = jnp.broadcast_to(ids_ref[...], (128, samples)).T
        wide_patch[...] = jnp.broadcast_to(patch_ref[...], (128, samples)).T

    ids = jnp.concatenate([wide_ids[...] - (base + i) * rows] * (rows // 128), axis=1)
    patch = jnp.concatenate([wide_patch[...]] * (rows // 128), axis=1)
    hit = lax.broadcasted_iota(jnp.int32, exp_ref.shape, 1) == ids
    weight = jnp.where(hit, patch, exp_ref[...].astype(f32)).astype(bf16)
    push = lax.dot_general(weight, emb_ref[...], (((0,), (0,)), ((), ())), preferred_element_type=f32)
    if final:
        push = push + other_ref[...].astype(f32)
        block = c_ref[...].astype(f32)
        inv = inverse_norm(block, 1)
        unit = block * inv
        push = (push - unit * jnp.sum(push * unit, axis=1, keepdims=True)) * inv
    out_ref[...] = push.astype(bf16)


def pushed(ids, patch, emb, exps, half, centers=None, other=None, rows=1024):
    samples, depth = emb.shape
    count = exps.shape[1] // 2
    base = half * (count // rows)
    final = centers is not None
    fixed = lambda i: (0, 0)
    step = lambda i: (i, 0)
    extra = (centers, other) if final else ()
    return pl.pallas_call(
        functools.partial(push_kernel, base, final),
        grid=(count // rows,),
        in_specs=[
            pl.BlockSpec((1, samples), fixed),
            pl.BlockSpec((1, samples), fixed),
            pl.BlockSpec((samples, depth), fixed),
            pl.BlockSpec((samples, rows), lambda i: (0, base + i)),
        ]
        + [pl.BlockSpec((rows, depth), step)] * len(extra),
        out_specs=pl.BlockSpec((rows, depth), step),
        out_shape=jax.ShapeDtypeStruct((count, depth), bf16),
        scratch_shapes=[pltpu.VMEM((samples, 128), jnp.int32), pltpu.VMEM((samples, 128), f32)],
        cost_estimate=pl.CostEstimate(
            flops=2 * count * depth * samples, bytes_accessed=2 * count * samples, transcendentals=0
        ),
    )(ids, patch, emb, exps, *extra)


def step(features, fc_weight, centers, labels):
    own, wide = features.shape
    class_rows, depth = centers.shape
    chips = lax.axis_size(CHIP)
    chip = lax.axis_index(CHIP)
    core = lax.axis_index(CORE)
    samples = chips * own

    other_centers = swapped(centers)
    cuts = tuple(range(0, wide, 1792)) + (wide,)
    embedded, parcel = embedded_rows(core.reshape(1), features, fc_weight, chips, cuts)
    x = to_chips(parcel).reshape(samples, depth + 256)

    by_core = labels.reshape(chips, 2, own)
    my_labels = jnp.where(core == 0, by_core[:, 0], by_core[:, 1]).reshape(1, samples)
    local = my_labels - chip * (2 * class_rows)
    inside = (local >= 0) & (local < 2 * class_rows)
    turned_ids = jnp.where(core == 0, local, (local + class_rows) % (2 * class_rows))
    ids = jnp.where(inside, turned_ids, -1)

    goal = target_directions(ids, own, centers, other_centers)
    early = 6
    exps, low, pull, emb_low, report, target_cos = exponentials(ids, x, goal, centers, other_centers, chips, early)
    report = to_chips(report)
    pull = pulled(exps, low, pull, early)
    parcel, scaled, patch, report = settled(ids, target_cos, report, pull, goal, emb_low)
    parcel = to_chips(parcel.reshape(chips, own, depth))

    other_push = pushed(ids, patch, scaled, exps, 1)
    other_push = swapped(other_push)
    grad_centers = pushed(ids, patch, scaled, exps, 0, centers, other_push)

    own_float = embedded.astype(f32)
    inv_emb = inverse_norm(own_float, 1)
    emb_dir = own_float * inv_emb
    grad_dir = jnp.sum(parcel.astype(f32), axis=0)
    grad_emb = (
        (grad_dir - emb_dir * jnp.sum(grad_dir * emb_dir, axis=1, keepdims=True)) * inv_emb
    ).astype(bf16)
    grads = from_chips(grad_emb).reshape(samples, depth)

    fcols = wide // (2 * chips)
    columns = x[:, depth:]
    both = lax.dot_general(columns, grads, (((0,), (0,)), ((), ())), preferred_element_type=f32)
    theirs_fc = swapped(both[128 : 128 + fcols])
    grad_fc = both[:fcols] + theirs_fc
    own_sums = lax.dynamic_slice_in_dim(report[0], chip * own, own)
    own_logits = lax.dynamic_slice_in_dim(report[0], samples + chip * own % 128, own)
    loss = jnp.log(own_sums) - own_logits
    return (loss, grad_centers, grad_fc)


def solution(mesh):
    torus = Mesh(mesh.devices.reshape(4, 4, 4, 2), CLS)
    placed = (P(CLS, None), P(), P(CLS, None), P())
    return jax.shard_map(
        step,
        mesh=torus,
        in_specs=placed,
        out_specs=(P(CLS), P(CLS, None), P(CLS, None)),
        check_vma=False,
    )
```

```python
import functools
import math

import jax
import jax.numpy as jnp
from jax import lax
from jax.experimental import pallas as pl
from jax.experimental.pallas import tpu as pltpu
from jax.sharding import Mesh
from jax.sharding import PartitionSpec as P


CLS = ("cls_0", "cls_1", "cls_2", "cls_3")
CHIP = ("cls_0", "cls_1", "cls_2")
CORE = "cls_3"

logit_scale = 64.0
cos_margin = math.cos(0.5)
sin_margin = math.sin(0.5)
epsilon = 1e-06

f32 = jnp.float32
bf16 = jnp.bfloat16


def swapped(x):
    return lax.ppermute(x, CORE, [(0, 1), (1, 0)])


def to_chips(x):
    return lax.all_to_all(x, CHIP, split_axis=0, concat_axis=0, tiled=True)


def from_chips(x):
    copies = jnp.broadcast_to(x, (lax.axis_size(CHIP), *x.shape))
    return lax.all_to_all(copies, CHIP, split_axis=0, concat_axis=0, tiled=True)


def inverse_norm(values, axis):
    return lax.rsqrt(jnp.sum(values * values, axis=axis, keepdims=True) + epsilon)


def margin(target_cos):
    target_sine = jnp.sqrt(1.0 - target_cos * target_cos)
    margined = target_cos * cos_margin - target_sine * sin_margin
    slope = cos_margin + sin_margin * target_cos / target_sine
    return margined, slope


ANY = pl.BlockSpec(memory_space=pl.ANY)
VMEM = pl.BlockSpec(memory_space=pltpu.VMEM)
SMEM = pl.BlockSpec(memory_space=pltpu.SMEM)


def embed_kernel(cuts, core_ref, f_ref, w_ref, out_ref, parcel_ref, weight, sems):
    copies = [
        pltpu.make_async_copy(w_ref.at[pl.ds(a, b - a)], weight.at[pl.ds(a, b - a)], sems.at[k])
        for k, (a, b) in enumerate(zip(cuts, cuts[1:]))
    ]
    for copy in copies:
        copy.start()
    chips = parcel_ref.shape[0]
    own, wide = f_ref.shape
    depth = out_ref.shape[1]
    fcols = wide // (2 * chips)
    lower = core_ref[0] == 0
    pad = jnp.zeros((own, 128 - fcols), bf16)
    for chip in range(chips):
        at = 2 * chip * fcols
        first = jnp.concatenate([f_ref[:, at : at + fcols], pad], axis=1)
        second = jnp.concatenate([f_ref[:, at + fcols : at + 2 * fcols], pad], axis=1)
        parcel_ref[chip, :, depth : depth + 128] = jnp.where(lower, first, second)
        parcel_ref[chip, :, depth + 128 :] = jnp.where(lower, second, first)
    total = None
    for copy, a, b in zip(copies, cuts, cuts[1:]):
        copy.wait()
        product = jnp.dot(f_ref[:, a:b], weight[a:b, :], preferred_element_type=f32)
        total = product if total is None else total + product
    rows = total.astype(bf16)
    out_ref[...] = rows
    for chip in range(chips):
        parcel_ref[chip, :, :depth] = rows


def embedded_rows(core, features, weight, chips, cuts):
    own, wide = features.shape
    depth = weight.shape[1]
    return pl.pallas_call(
        functools.partial(embed_kernel, cuts),
        in_specs=[SMEM, VMEM, ANY],
        out_specs=[VMEM, VMEM],
        out_shape=[
            jax.ShapeDtypeStruct((own, depth), bf16),
            jax.ShapeDtypeStruct((chips, own, depth + 256), bf16),
        ],
        scratch_shapes=[pltpu.VMEM((wide, depth), bf16), pltpu.SemaphoreType.DMA((len(cuts) - 1,))],
        cost_estimate=pl.CostEstimate(
            flops=2 * own * wide * depth, bytes_accessed=2 * wide * depth, transcendentals=0
        ),
        name="embed",
    )(core, features, weight)


def centers_kernel(batch, rows, ids_ref, busy_ref, own_ref, other_ref, low_ref, goal_ref, centers, found, in_sems,
                   out_sems):
    count, depth = own_ref.shape
    steps = 2 * count // rows

    def arrival(i):
        source = own_ref if i * rows < count else other_ref
        return pltpu.make_async_copy(
            source.at[pl.ds(i * rows % count, rows)], centers.at[pl.ds(i * rows, rows)], in_sems.at[i]
        )

    def departure(i):
        span = pl.ds(i * rows, rows)
        return pltpu.make_async_copy(centers.at[span], low_ref.at[span], out_sems.at[i])

    for i in range(steps):
        arrival(i).start()
    found[...] = jnp.zeros_like(found)
    for i in range(steps):
        arrival(i).wait()
        block = centers[i * rows : (i + 1) * rows, :].astype(f32)
        centers[i * rows : (i + 1) * rows, :] = (block * inverse_norm(block, 1)).astype(bf16)
        if i > 0:
            departure(i - 1).start()
    spot = lax.broadcasted_iota(jnp.int32, (16, depth), 0)

    def group(g, carry):
        @pl.when(busy_ref[g] >= 0)
        def _():
            def sample(b, carry):
                at = g * batch + b
                row = ids_ref[0, at]

                @pl.when(row >= 0)
                def _():
                    near = centers[pl.ds(pl.multiple_of(row // 16 * 16, 16), 16), :].astype(f32)
                    found[pl.ds(at, 1), :] = jnp.sum(jnp.where(spot == row % 16, near, 0.0), axis=0, keepdims=True)

                return carry

            lax.fori_loop(0, batch, sample, 0)

        return carry

    lax.fori_loop(0, busy_ref.shape[0], group, 0)
    departure(steps - 1).start()
    goal_ref[...] = found[...].astype(bf16)
    for i in range(steps):
        departure(i).wait()


def center_directions(ids, batch, own, other, rows=1024):
    count, depth = own.shape
    samples = ids.shape[1]
    steps = 2 * count // rows
    busy = jnp.max(ids.reshape(samples // batch, batch), axis=1)
    return pl.pallas_call(
        functools.partial(centers_kernel, batch, rows),
        in_specs=[SMEM, SMEM, ANY, ANY],
        out_specs=[ANY, VMEM],
        out_shape=[
            jax.ShapeDtypeStruct((2 * count, depth), bf16),
            jax.ShapeDtypeStruct((samples, depth), bf16),
        ],
        scratch_shapes=[
            pltpu.VMEM((2 * count, depth), bf16),
            pltpu.VMEM((samples, depth), f32),
            pltpu.SemaphoreType.DMA((steps,)),
            pltpu.SemaphoreType.DMA((steps,)),
        ],
        cost_estimate=pl.CostEstimate(
            flops=2 * count * depth * samples, bytes_accessed=8 * count * depth, transcendentals=0
        ),
        name="targets",
    )(ids, busy, own, other)


def row_of(values):
    part = values[:, :128]
    for k in range(1, values.shape[1] // 128):
        part = part + values[:, k * 128 : (k + 1) * 128]
    return jnp.sum(part.T, axis=0, keepdims=True)


def exp_kernel(early, lanes, ids_ref, x_ref, goal_ref, low_ref, exp_ref, pull_ref, emb_ref,
               report_ref, cos_ref, wide_ids, scaled, row_sum, total):
    i = pl.program_id(0)
    rows = low_ref.shape[0]
    samples = x_ref.shape[0]
    sub = samples // lanes

    @pl.when(i == 0)
    def _():
        wide_ids[...] = jnp.broadcast_to(ids_ref[...], (128, samples)).T
        x = x_ref[...].astype(f32)
        emb = (x * inverse_norm(x, 1)).astype(bf16)
        emb_ref[...] = emb
        scaled[...] = (emb * logit_scale).astype(bf16)
        row_sum[...] = jnp.zeros_like(row_sum)
        total[...] = jnp.zeros_like(total)

    def chunk(with_pull):
        columns = lax.broadcasted_iota(jnp.int32, (sub, 128), 1)

        def products(m):
            return lax.dot_general(
                scaled[m * sub : (m + 1) * sub, :],
                low_ref[...],
                (((1,), (1,)), ((), ())),
                preferred_element_type=f32,
            )

        logits = products(0)
        for m in range(lanes):
            later = products(m + 1) if m + 1 < lanes else None
            span = slice(m * sub, (m + 1) * sub)
            ids = wide_ids[span, :] - i * rows
            part = None
            for t in range(rows // 128):
                weight = jnp.exp(logits[:, t * 128 : (t + 1) * 128])
                weight = jnp.where(columns + t * 128 == ids, 0.0, weight)
                part = weight if part is None else part + weight
                exp_ref[span, t * 128 : (t + 1) * 128] = weight.astype(bf16)
            row_sum[span, :] += part
            if with_pull:
                total[span, :] += jnp.dot(exp_ref[span, :], low_ref[...], preferred_element_type=f32)
            logits = later

    @pl.when(i < early)
    def _():
        chunk(True)

    @pl.when(i >= early)
    def _():
        chunk(False)

    @pl.when(i == early)
    def _():
        pull_ref[...] = total[...]

    @pl.when(i == pl.num_programs(0) - 1)
    def _():
        target_cos = row_of(goal_ref[...].astype(f32) * scaled[...].astype(f32)) * (1.0 / logit_scale)
        cos_ref[...] = target_cos
        margined, _ = margin(target_cos)
        is_here = ids_ref[...] >= 0
        logit = jnp.where(is_here, logit_scale * margined, 0.0)
        sums = row_of(row_sum[...]) + jnp.where(is_here, jnp.exp(logit_scale * margined), 0.0)
        chips = report_ref.shape[0]
        own = samples // chips
        lane = lax.broadcasted_iota(jnp.int32, (1, 128), 1)
        for chip in range(chips):
            k = chip * own // 128
            theirs = (lane + k * 128) // own == chip
            report_ref[chip, :, :samples] = sums
            report_ref[chip, :, samples:] = jnp.where(theirs, logit[:, k * 128 : (k + 1) * 128], 0.0)


def exponentials(ids, x, goal, low, chips, early, rows=1024, lanes=2):
    samples = x.shape[0]
    count, depth = low.shape
    fixed = lambda i: (0, 0)
    return pl.pallas_call(
        functools.partial(exp_kernel, early, lanes),
        grid=(count // rows,),
        in_specs=[
            pl.BlockSpec((1, samples), fixed),
            pl.BlockSpec((samples, depth), fixed),
            pl.BlockSpec((samples, depth), fixed),
            pl.BlockSpec((rows, depth), lambda i: (i, 0)),
        ],
        out_specs=[
            pl.BlockSpec((samples, rows), lambda i: (0, i)),
            pl.BlockSpec((samples, depth), fixed),
            pl.BlockSpec((samples, depth), fixed),
            pl.BlockSpec((chips, 1, samples + 128), lambda i: (0, 0, 0)),
            pl.BlockSpec((1, samples), fixed),
        ],
        out_shape=[
            jax.ShapeDtypeStruct((samples, count), bf16),
            jax.ShapeDtypeStruct((samples, depth), f32),
            jax.ShapeDtypeStruct((samples, depth), bf16),
            jax.ShapeDtypeStruct((chips, 1, samples + 128), f32),
            jax.ShapeDtypeStruct((1, samples), f32),
        ],
        scratch_shapes=[
            pltpu.VMEM((samples, 128), jnp.int32),
            pltpu.VMEM((samples, depth), bf16),
            pltpu.VMEM((samples, 128), f32),
            pltpu.VMEM((samples, depth), f32),
        ],
        cost_estimate=pl.CostEstimate(
            flops=2 * count * depth * samples,
            bytes_accessed=4 * count * depth,
            transcendentals=count * samples,
        ),
        name="exponentials",
    )(ids, x, goal, low)


def pull_kernel(early, rows, exp_ref, low_ref, start_ref, out_ref, exps, lows, exp_sems, low_sems, start_sem):
    steps = low_ref.shape[0] // rows - early
    start = pltpu.make_async_copy(start_ref, out_ref, start_sem)

    def fetch(i, slot):
        return (
            pltpu.make_async_copy(
                exp_ref.at[:, pl.ds((early + i) * rows, rows)], exps.at[slot], exp_sems.at[slot]
            ),
            pltpu.make_async_copy(low_ref.at[pl.ds((early + i) * rows, rows)], lows.at[slot], low_sems.at[slot]),
        )

    for i in range(steps):
        for copy in fetch(i, i):
            copy.start()
        if i == 0:
            start.start()
    for i in range(steps):
        for copy in fetch(i, i):
            copy.wait()
        if i == 0:
            start.wait()
        out_ref[...] += jnp.dot(exps[i], lows[i], preferred_element_type=f32)


def pulled(exps, low, start, early, rows=1024):
    samples = exps.shape[0]
    count, depth = low.shape
    steps = count // rows - early
    return pl.pallas_call(
        functools.partial(pull_kernel, early, rows),
        in_specs=[ANY, ANY, ANY],
        out_specs=VMEM,
        out_shape=jax.ShapeDtypeStruct((samples, depth), f32),
        scratch_shapes=[
            pltpu.VMEM((steps, samples, rows), bf16),
            pltpu.VMEM((steps, rows, depth), bf16),
            pltpu.SemaphoreType.DMA((steps,)),
            pltpu.SemaphoreType.DMA((steps,)),
            pltpu.SemaphoreType.DMA,
        ],
        cost_estimate=pl.CostEstimate(
            flops=2 * steps * rows * depth * samples,
            bytes_accessed=2 * steps * rows * (depth + samples),
            transcendentals=0,
        ),
        name="pull",
    )(exps, low, start)


def settle_kernel(ids_ref, cos_ref, report_ref, pull_ref, goal_ref, emb_ref, parcel_ref, scaled_ref,
                  patch_ref, sums_ref, wide_scale, wide_target):
    i = pl.program_id(0)
    rows, depth = goal_ref.shape
    samples = ids_ref.shape[1]

    @pl.when(i == 0)
    def _():
        report = jnp.sum(report_ref[...], axis=0)
        sums_ref[...] = report
        sums = report[:, :samples]
        margined, slope = margin(cos_ref[...])
        patch = slope * (jnp.exp(logit_scale * margined) - sums)
        patch_ref[...] = patch
        scale = logit_scale / sums
        at_target = jnp.where(ids_ref[...] >= 0, scale * patch, 0.0)
        wide_scale[...] = jnp.broadcast_to(scale, (128, samples)).T
        wide_target[...] = jnp.broadcast_to(at_target, (128, samples)).T

    span = pl.ds(pl.multiple_of(i * rows, rows), rows)
    scale = jnp.concatenate([wide_scale[span, :]] * (depth // 128), axis=1)
    at_target = jnp.concatenate([wide_target[span, :]] * (depth // 128), axis=1)
    parcel_ref[...] = (pull_ref[...] * scale + at_target * goal_ref[...].astype(f32)).astype(bf16)
    scaled_ref[...] = (emb_ref[...].astype(f32) * scale).astype(bf16)


def settled(ids, target_cos, report, pull, goal, emb, rows=512):
    samples, depth = emb.shape
    fixed = lambda i: (0, 0)
    step = lambda i: (i, 0)
    row = pl.BlockSpec((1, samples), fixed)
    return pl.pallas_call(
        settle_kernel,
        grid=(samples // rows,),
        in_specs=[row, row, pl.BlockSpec(report.shape, lambda i: (0, 0, 0))]
        + [pl.BlockSpec((rows, depth), step)] * 3,
        out_specs=[
            pl.BlockSpec((rows, depth), step),
            pl.BlockSpec((rows, depth), step),
            row,
            pl.BlockSpec((1, report.shape[2]), fixed),
        ],
        out_shape=[
            jax.ShapeDtypeStruct((samples, depth), bf16),
            jax.ShapeDtypeStruct((samples, depth), bf16),
            jax.ShapeDtypeStruct((1, samples), f32),
            jax.ShapeDtypeStruct((1, report.shape[2]), f32),
        ],
        scratch_shapes=[pltpu.VMEM((samples, 128), f32), pltpu.VMEM((samples, 128), f32)],
        cost_estimate=pl.CostEstimate(
            flops=8 * samples * depth, bytes_accessed=14 * samples * depth, transcendentals=0
        ),
        name="settle",
    )(ids, target_cos, report, pull, goal, emb)


def push_kernel(base, final, ids_ref, patch_ref, emb_ref, exp_ref, *refs):
    i = pl.program_id(0)
    samples, rows = exp_ref.shape
    if final:
        c_ref, other_ref, out_ref, wide_ids, wide_patch = refs
    else:
        out_ref, wide_ids, wide_patch = refs

    @pl.when(i == 0)
    def _():
        wide_ids[...] = jnp.broadcast_to(ids_ref[...], (128, samples)).T
        wide_patch[...] = jnp.broadcast_to(patch_ref[...], (128, samples)).T

    ids = jnp.concatenate([wide_ids[...] - (base + i) * rows] * (rows // 128), axis=1)
    patch = jnp.concatenate([wide_patch[...]] * (rows // 128), axis=1)
    hit = lax.broadcasted_iota(jnp.int32, exp_ref.shape, 1) == ids
    weight = jnp.where(hit, patch, exp_ref[...].astype(f32)).astype(bf16)
    push = lax.dot_general(weight, emb_ref[...], (((0,), (0,)), ((), ())), preferred_element_type=f32)
    if final:
        push = push + other_ref[...].astype(f32)
        block = c_ref[...].astype(f32)
        inv = inverse_norm(block, 1)
        unit = block * inv
        push = (push - unit * jnp.sum(push * unit, axis=1, keepdims=True)) * inv
    out_ref[...] = push.astype(bf16)


def pushed(ids, patch, emb, exps, half, centers=None, other=None, rows=1024):
    samples, depth = emb.shape
    count = exps.shape[1] // 2
    base = half * (count // rows)
    final = centers is not None
    fixed = lambda i: (0, 0)
    step = lambda i: (i, 0)
    extra = (centers, other) if final else ()
    return pl.pallas_call(
        functools.partial(push_kernel, base, final),
        grid=(count // rows,),
        in_specs=[
            pl.BlockSpec((1, samples), fixed),
            pl.BlockSpec((1, samples), fixed),
            pl.BlockSpec((samples, depth), fixed),
            pl.BlockSpec((samples, rows), lambda i: (0, base + i)),
        ]
        + [pl.BlockSpec((rows, depth), step)] * len(extra),
        out_specs=pl.BlockSpec((rows, depth), step),
        out_shape=jax.ShapeDtypeStruct((count, depth), bf16),
        scratch_shapes=[pltpu.VMEM((samples, 128), jnp.int32), pltpu.VMEM((samples, 128), f32)],
        cost_estimate=pl.CostEstimate(
            flops=2 * count * depth * samples, bytes_accessed=2 * count * samples, transcendentals=0
        ),
    )(ids, patch, emb, exps, *extra)


def step(features, fc_weight, centers, labels):
    own, wide = features.shape
    class_rows, depth = centers.shape
    chips = lax.axis_size(CHIP)
    chip = lax.axis_index(CHIP)
    core = lax.axis_index(CORE)
    samples = chips * own

    other_centers = swapped(centers)
    cuts = tuple(range(0, wide, 1792)) + (wide,)
    embedded, parcel = embedded_rows(core.reshape(1), features, fc_weight, chips, cuts)
    x = to_chips(parcel).reshape(samples, depth + 256)

    by_core = labels.reshape(chips, 2, own)
    my_labels = jnp.where(core == 0, by_core[:, 0], by_core[:, 1]).reshape(1, samples)
    local = my_labels - chip * (2 * class_rows)
    inside = (local >= 0) & (local < 2 * class_rows)
    turned_ids = jnp.where(core == 0, local, (local + class_rows) % (2 * class_rows))
    ids = jnp.where(inside, turned_ids, -1)

    low, goal = center_directions(ids, own, centers, other_centers)
    early = 6
    exps, pull, emb_low, report, target_cos = exponentials(ids, x, goal, low, chips, early)
    report = to_chips(report)
    pull = pulled(exps, low, pull, early)
    parcel, scaled, patch, report = settled(ids, target_cos, report, pull, goal, emb_low)
    parcel = to_chips(parcel.reshape(chips, own, depth))

    other_push = pushed(ids, patch, scaled, exps, 1)
    other_push = swapped(other_push)
    grad_centers = pushed(ids, patch, scaled, exps, 0, centers, other_push)

    own_float = embedded.astype(f32)
    inv_emb = inverse_norm(own_float, 1)
    emb_dir = own_float * inv_emb
    grad_dir = jnp.sum(parcel.astype(f32), axis=0)
    grad_emb = (
        (grad_dir - emb_dir * jnp.sum(grad_dir * emb_dir, axis=1, keepdims=True)) * inv_emb
    ).astype(bf16)
    grads = from_chips(grad_emb).reshape(samples, depth)

    fcols = wide // (2 * chips)
    columns = x[:, depth:]
    both = lax.dot_general(columns, grads, (((0,), (0,)), ((), ())), preferred_element_type=f32)
    theirs_fc = swapped(both[128 : 128 + fcols])
    grad_fc = both[:fcols] + theirs_fc
    own_sums = lax.dynamic_slice_in_dim(report[0], chip * own, own)
    own_logits = lax.dynamic_slice_in_dim(report[0], samples + chip * own % 128, own)
    loss = jnp.log(own_sums) - own_logits
    return (loss, grad_centers, grad_fc)


def solution(mesh):
    torus = Mesh(mesh.devices.reshape(4, 4, 4, 2), CLS)
    placed = (P(CLS, None), P(), P(CLS, None), P())
    return jax.shard_map(
        step,
        mesh=torus,
        in_specs=placed,
        out_specs=(P(CLS), P(CLS, None), P(CLS, None)),
        check_vma=False,
    )
```

```python
import functools
import math

import jax
import jax.numpy as jnp
from jax import lax
from jax.experimental import pallas as pl
from jax.experimental.pallas import tpu as pltpu
from jax.sharding import Mesh
from jax.sharding import PartitionSpec as P


CLS = ("cls_0", "cls_1", "cls_2", "cls_3")
CHIP = ("cls_0", "cls_1", "cls_2")
CORE = "cls_3"

logit_scale = 64.0
cos_margin = math.cos(0.5)
sin_margin = math.sin(0.5)
epsilon = 1e-06

f32 = jnp.float32
bf16 = jnp.bfloat16


def swapped(x):
    return lax.ppermute(x, CORE, [(0, 1), (1, 0)])


def to_chips(x):
    return lax.all_to_all(x, CHIP, split_axis=0, concat_axis=0, tiled=True)


def from_chips(x):
    copies = jnp.broadcast_to(x, (lax.axis_size(CHIP), *x.shape))
    return lax.all_to_all(copies, CHIP, split_axis=0, concat_axis=0, tiled=True)


def inverse_norm(values, axis):
    return lax.rsqrt(jnp.sum(values * values, axis=axis, keepdims=True) + epsilon)


def margin(target_cos):
    target_sine = jnp.sqrt(1.0 - target_cos * target_cos)
    margined = target_cos * cos_margin - target_sine * sin_margin
    slope = cos_margin + sin_margin * target_cos / target_sine
    return margined, slope


ANY = pl.BlockSpec(memory_space=pl.ANY)
VMEM = pl.BlockSpec(memory_space=pltpu.VMEM)
SMEM = pl.BlockSpec(memory_space=pltpu.SMEM)


def embed_kernel(cuts, core_ref, f_ref, w_ref, out_ref, parcel_ref, weight, sems):
    copies = [
        pltpu.make_async_copy(w_ref.at[pl.ds(a, b - a)], weight.at[pl.ds(a, b - a)], sems.at[k])
        for k, (a, b) in enumerate(zip(cuts, cuts[1:]))
    ]
    for copy in copies:
        copy.start()
    chips = parcel_ref.shape[0]
    own, wide = f_ref.shape
    depth = out_ref.shape[1]
    fcols = wide // (2 * chips)
    lower = core_ref[0] == 0
    pad = jnp.zeros((own, 128 - fcols), bf16)
    for chip in range(chips):
        at = 2 * chip * fcols
        first = jnp.concatenate([f_ref[:, at : at + fcols], pad], axis=1)
        second = jnp.concatenate([f_ref[:, at + fcols : at + 2 * fcols], pad], axis=1)
        parcel_ref[chip, :, depth : depth + 128] = jnp.where(lower, first, second)
        parcel_ref[chip, :, depth + 128 :] = jnp.where(lower, second, first)
    total = None
    for copy, a, b in zip(copies, cuts, cuts[1:]):
        copy.wait()
        product = jnp.dot(f_ref[:, a:b], weight[a:b, :], preferred_element_type=f32)
        total = product if total is None else total + product
    rows = total.astype(bf16)
    out_ref[...] = rows
    rows = rows.astype(f32)
    low = (rows * inverse_norm(rows, 1)).astype(bf16)
    for chip in range(chips):
        parcel_ref[chip, :, :depth] = low


def embedded_rows(core, features, weight, chips, cuts):
    own, wide = features.shape
    depth = weight.shape[1]
    return pl.pallas_call(
        functools.partial(embed_kernel, cuts),
        in_specs=[SMEM, VMEM, ANY],
        out_specs=[VMEM, VMEM],
        out_shape=[
            jax.ShapeDtypeStruct((own, depth), bf16),
            jax.ShapeDtypeStruct((chips, own, depth + 256), bf16),
        ],
        scratch_shapes=[pltpu.VMEM((wide, depth), bf16), pltpu.SemaphoreType.DMA((len(cuts) - 1,))],
        cost_estimate=pl.CostEstimate(
            flops=2 * own * wide * depth, bytes_accessed=2 * wide * depth, transcendentals=0
        ),
        name="embed",
    )(core, features, weight)


def centers_kernel(batch, rows, ids_ref, busy_ref, own_ref, other_ref, low_ref, goal_ref, centers, found, in_sems,
                   out_sems):
    count, depth = own_ref.shape
    steps = 2 * count // rows

    def arrival(i):
        source = own_ref if i * rows < count else other_ref
        return pltpu.make_async_copy(
            source.at[pl.ds(i * rows % count, rows)], centers.at[pl.ds(i * rows, rows)], in_sems.at[i]
        )

    def departure(i):
        span = pl.ds(i * rows, rows)
        return pltpu.make_async_copy(centers.at[span], low_ref.at[span], out_sems.at[i])

    for i in range(steps):
        arrival(i).start()
    found[...] = jnp.zeros_like(found)
    for i in range(steps):
        arrival(i).wait()
        block = centers[i * rows : (i + 1) * rows, :].astype(f32)
        centers[i * rows : (i + 1) * rows, :] = (block * inverse_norm(block, 1)).astype(bf16)
        if i > 0:
            departure(i - 1).start()
    spot = lax.broadcasted_iota(jnp.int32, (16, depth), 0)

    def group(g, carry):
        @pl.when(busy_ref[g] >= 0)
        def _():
            def sample(b, carry):
                at = g * batch + b
                row = ids_ref[0, at]

                @pl.when(row >= 0)
                def _():
                    near = centers[pl.ds(pl.multiple_of(row // 16 * 16, 16), 16), :].astype(f32)
                    found[pl.ds(at, 1), :] = jnp.sum(jnp.where(spot == row % 16, near, 0.0), axis=0, keepdims=True)

                return carry

            lax.fori_loop(0, batch, sample, 0)

        return carry

    lax.fori_loop(0, busy_ref.shape[0], group, 0)
    departure(steps - 1).start()
    goal_ref[...] = found[...].astype(bf16)
    for i in range(steps):
        departure(i).wait()


def center_directions(ids, batch, own, other, rows=1024):
    count, depth = own.shape
    samples = ids.shape[1]
    steps = 2 * count // rows
    busy = jnp.max(ids.reshape(samples // batch, batch), axis=1)
    return pl.pallas_call(
        functools.partial(centers_kernel, batch, rows),
        in_specs=[SMEM, SMEM, ANY, ANY],
        out_specs=[ANY, VMEM],
        out_shape=[
            jax.ShapeDtypeStruct((2 * count, depth), bf16),
            jax.ShapeDtypeStruct((samples, depth), bf16),
        ],
        scratch_shapes=[
            pltpu.VMEM((2 * count, depth), bf16),
            pltpu.VMEM((samples, depth), f32),
            pltpu.SemaphoreType.DMA((steps,)),
            pltpu.SemaphoreType.DMA((steps,)),
        ],
        cost_estimate=pl.CostEstimate(
            flops=2 * count * depth * samples, bytes_accessed=8 * count * depth, transcendentals=0
        ),
        name="targets",
    )(ids, busy, own, other)


def row_of(values):
    part = values[:, :128]
    for k in range(1, values.shape[1] // 128):
        part = part + values[:, k * 128 : (k + 1) * 128]
    return jnp.sum(part.T, axis=0, keepdims=True)


def exp_kernel(early, lanes, ids_ref, x_ref, goal_ref, low_ref, exp_ref, pull_ref,
               report_ref, cos_ref, wide_ids, scaled, row_sum, total):
    i = pl.program_id(0)
    rows = low_ref.shape[0]
    samples = x_ref.shape[0]
    sub = samples // lanes

    @pl.when(i == 0)
    def _():
        wide_ids[...] = jnp.broadcast_to(ids_ref[...], (128, samples)).T
        scaled[...] = (x_ref[...].astype(f32) * logit_scale).astype(bf16)
        row_sum[...] = jnp.zeros_like(row_sum)
        total[...] = jnp.zeros_like(total)

    def chunk(with_pull):
        columns = lax.broadcasted_iota(jnp.int32, (sub, 128), 1)

        def products(m):
            return lax.dot_general(
                scaled[m * sub : (m + 1) * sub, :],
                low_ref[...],
                (((1,), (1,)), ((), ())),
                preferred_element_type=f32,
            )

        logits = products(0)
        for m in range(lanes):
            later = products(m + 1) if m + 1 < lanes else None
            span = slice(m * sub, (m + 1) * sub)
            ids = wide_ids[span, :] - i * rows
            part = None
            for t in range(rows // 128):
                weight = jnp.exp(logits[:, t * 128 : (t + 1) * 128])
                weight = jnp.where(columns + t * 128 == ids, 0.0, weight)
                part = weight if part is None else part + weight
                exp_ref[span, t * 128 : (t + 1) * 128] = weight.astype(bf16)
            row_sum[span, :] += part
            if with_pull:
                total[span, :] += jnp.dot(exp_ref[span, :], low_ref[...], preferred_element_type=f32)
            logits = later

    @pl.when(i < early)
    def _():
        chunk(True)

    @pl.when(i >= early)
    def _():
        chunk(False)

    @pl.when(i == early)
    def _():
        pull_ref[...] = total[...]

    @pl.when(i == pl.num_programs(0) - 1)
    def _():
        target_cos = row_of(goal_ref[...].astype(f32) * scaled[...].astype(f32)) * (1.0 / logit_scale)
        cos_ref[...] = target_cos
        margined, _ = margin(target_cos)
        is_here = ids_ref[...] >= 0
        logit = jnp.where(is_here, logit_scale * margined, 0.0)
        sums = row_of(row_sum[...]) + jnp.where(is_here, jnp.exp(logit_scale * margined), 0.0)
        chips = report_ref.shape[0]
        own = samples // chips
        lane = lax.broadcasted_iota(jnp.int32, (1, 128), 1)
        for chip in range(chips):
            k = chip * own // 128
            theirs = (lane + k * 128) // own == chip
            report_ref[chip, :, :samples] = sums
            report_ref[chip, :, samples:] = jnp.where(theirs, logit[:, k * 128 : (k + 1) * 128], 0.0)


def exponentials(ids, x, goal, low, chips, early, rows=1024, lanes=2):
    samples = x.shape[0]
    count, depth = low.shape
    fixed = lambda i: (0, 0)
    return pl.pallas_call(
        functools.partial(exp_kernel, early, lanes),
        grid=(count // rows,),
        in_specs=[
            pl.BlockSpec((1, samples), fixed),
            pl.BlockSpec((samples, depth), fixed),
            pl.BlockSpec((samples, depth), fixed),
            pl.BlockSpec((rows, depth), lambda i: (i, 0)),
        ],
        out_specs=[
            pl.BlockSpec((samples, rows), lambda i: (0, i)),
            pl.BlockSpec((samples, depth), fixed),
            pl.BlockSpec((chips, 1, samples + 128), lambda i: (0, 0, 0)),
            pl.BlockSpec((1, samples), fixed),
        ],
        out_shape=[
            jax.ShapeDtypeStruct((samples, count), bf16),
            jax.ShapeDtypeStruct((samples, depth), f32),
            jax.ShapeDtypeStruct((chips, 1, samples + 128), f32),
            jax.ShapeDtypeStruct((1, samples), f32),
        ],
        scratch_shapes=[
            pltpu.VMEM((samples, 128), jnp.int32),
            pltpu.VMEM((samples, depth), bf16),
            pltpu.VMEM((samples, 128), f32),
            pltpu.VMEM((samples, depth), f32),
        ],
        cost_estimate=pl.CostEstimate(
            flops=2 * count * depth * samples,
            bytes_accessed=4 * count * depth,
            transcendentals=count * samples,
        ),
        name="exponentials",
    )(ids, x, goal, low)


def pull_kernel(early, rows, exp_ref, low_ref, start_ref, out_ref, exps, lows, exp_sems, low_sems, start_sem):
    steps = low_ref.shape[0] // rows - early
    start = pltpu.make_async_copy(start_ref, out_ref, start_sem)

    def fetch(i, slot):
        return (
            pltpu.make_async_copy(
                exp_ref.at[:, pl.ds((early + i) * rows, rows)], exps.at[slot], exp_sems.at[slot]
            ),
            pltpu.make_async_copy(low_ref.at[pl.ds((early + i) * rows, rows)], lows.at[slot], low_sems.at[slot]),
        )

    for i in range(steps):
        for copy in fetch(i, i):
            copy.start()
        if i == 0:
            start.start()
    for i in range(steps):
        for copy in fetch(i, i):
            copy.wait()
        if i == 0:
            start.wait()
        out_ref[...] += jnp.dot(exps[i], lows[i], preferred_element_type=f32)


def pulled(exps, low, start, early, rows=1024):
    samples = exps.shape[0]
    count, depth = low.shape
    steps = count // rows - early
    return pl.pallas_call(
        functools.partial(pull_kernel, early, rows),
        in_specs=[ANY, ANY, ANY],
        out_specs=VMEM,
        out_shape=jax.ShapeDtypeStruct((samples, depth), f32),
        scratch_shapes=[
            pltpu.VMEM((steps, samples, rows), bf16),
            pltpu.VMEM((steps, rows, depth), bf16),
            pltpu.SemaphoreType.DMA((steps,)),
            pltpu.SemaphoreType.DMA((steps,)),
            pltpu.SemaphoreType.DMA,
        ],
        cost_estimate=pl.CostEstimate(
            flops=2 * steps * rows * depth * samples,
            bytes_accessed=2 * steps * rows * (depth + samples),
            transcendentals=0,
        ),
        name="pull",
    )(exps, low, start)


def settle_kernel(ids_ref, cos_ref, report_ref, pull_ref, goal_ref, emb_ref, parcel_ref, scaled_ref,
                  patch_ref, sums_ref, wide_scale, wide_target):
    i = pl.program_id(0)
    rows, depth = goal_ref.shape
    samples = ids_ref.shape[1]

    @pl.when(i == 0)
    def _():
        report = jnp.sum(report_ref[...], axis=0)
        sums_ref[...] = report
        sums = report[:, :samples]
        margined, slope = margin(cos_ref[...])
        patch = slope * (jnp.exp(logit_scale * margined) - sums)
        patch_ref[...] = patch
        scale = logit_scale / sums
        at_target = jnp.where(ids_ref[...] >= 0, scale * patch, 0.0)
        wide_scale[...] = jnp.broadcast_to(scale, (128, samples)).T
        wide_target[...] = jnp.broadcast_to(at_target, (128, samples)).T

    span = pl.ds(pl.multiple_of(i * rows, rows), rows)
    scale = jnp.concatenate([wide_scale[span, :]] * (depth // 128), axis=1)
    at_target = jnp.concatenate([wide_target[span, :]] * (depth // 128), axis=1)
    parcel_ref[...] = (pull_ref[...] * scale + at_target * goal_ref[...].astype(f32)).astype(bf16)
    scaled_ref[...] = (emb_ref[...].astype(f32) * scale).astype(bf16)


def settled(ids, target_cos, report, pull, goal, emb, rows=512):
    samples, depth = goal.shape
    fixed = lambda i: (0, 0)
    step = lambda i: (i, 0)
    row = pl.BlockSpec((1, samples), fixed)
    return pl.pallas_call(
        settle_kernel,
        grid=(samples // rows,),
        in_specs=[row, row, pl.BlockSpec(report.shape, lambda i: (0, 0, 0))]
        + [pl.BlockSpec((rows, depth), step)] * 3,
        out_specs=[
            pl.BlockSpec((rows, depth), step),
            pl.BlockSpec((rows, depth), step),
            row,
            pl.BlockSpec((1, report.shape[2]), fixed),
        ],
        out_shape=[
            pltpu.HBM((samples, depth), bf16),
            pltpu.HBM((samples, depth), bf16),
            pltpu.HBM((1, samples), f32),
            pltpu.HBM((1, report.shape[2]), f32),
        ],
        scratch_shapes=[pltpu.VMEM((samples, 128), f32), pltpu.VMEM((samples, 128), f32)],
        compiler_params=pltpu.CompilerParams(vmem_limit_bytes=24 * 1024 * 1024),
        cost_estimate=pl.CostEstimate(
            flops=8 * samples * depth, bytes_accessed=14 * samples * depth, transcendentals=0
        ),
        name="settle",
    )(ids, target_cos, report, pltpu.with_memory_space_constraint(pull, pltpu.HBM), goal, emb)


def push_kernel(base, final, ids_ref, patch_ref, emb_ref, exp_ref, *refs):
    i = pl.program_id(0)
    samples, rows = exp_ref.shape
    if final:
        c_ref, other_ref, out_ref, wide_ids, wide_patch = refs
    else:
        out_ref, wide_ids, wide_patch = refs

    @pl.when(i == 0)
    def _():
        wide_ids[...] = jnp.broadcast_to(ids_ref[...], (128, samples)).T
        wide_patch[...] = jnp.broadcast_to(patch_ref[...], (128, samples)).T

    ids = jnp.concatenate([wide_ids[...] - (base + i) * rows] * (rows // 128), axis=1)
    patch = jnp.concatenate([wide_patch[...]] * (rows // 128), axis=1)
    hit = lax.broadcasted_iota(jnp.int32, exp_ref.shape, 1) == ids
    weight = jnp.where(hit, patch, exp_ref[...].astype(f32)).astype(bf16)
    push = lax.dot_general(weight, emb_ref[...], (((0,), (0,)), ((), ())), preferred_element_type=f32)
    if final:
        push = push + other_ref[...].astype(f32)
        block = c_ref[...].astype(f32)
        inv = inverse_norm(block, 1)
        unit = block * inv
        push = (push - unit * jnp.sum(push * unit, axis=1, keepdims=True)) * inv
    out_ref[...] = push.astype(bf16)


def pushed(ids, patch, emb, exps, half, centers=None, other=None, rows=1024):
    samples, depth = emb.shape
    count = exps.shape[1] // 2
    base = half * (count // rows)
    final = centers is not None
    fixed = lambda i: (0, 0)
    step = lambda i: (i, 0)
    extra = (centers, other) if final else ()
    return pl.pallas_call(
        functools.partial(push_kernel, base, final),
        grid=(count // rows,),
        in_specs=[
            pl.BlockSpec((1, samples), fixed),
            pl.BlockSpec((1, samples), fixed),
            pl.BlockSpec((samples, depth), fixed),
            pl.BlockSpec((samples, rows), lambda i: (0, base + i)),
        ]
        + [pl.BlockSpec((rows, depth), step)] * len(extra),
        out_specs=pl.BlockSpec((rows, depth), step),
        out_shape=jax.ShapeDtypeStruct((count, depth), bf16),
        scratch_shapes=[pltpu.VMEM((samples, 128), jnp.int32), pltpu.VMEM((samples, 128), f32)],
        cost_estimate=pl.CostEstimate(
            flops=2 * count * depth * samples, bytes_accessed=2 * count * samples, transcendentals=0
        ),
    )(ids, patch, emb, exps, *extra)


def step(features, fc_weight, centers, labels):
    own, wide = features.shape
    class_rows, depth = centers.shape
    chips = lax.axis_size(CHIP)
    chip = lax.axis_index(CHIP)
    core = lax.axis_index(CORE)
    samples = chips * own

    other_centers = swapped(centers)
    cuts = tuple(range(0, wide, 1792)) + (wide,)
    embedded, parcel = embedded_rows(core.reshape(1), features, fc_weight, chips, cuts)
    x = to_chips(parcel).reshape(samples, depth + 256)

    by_core = labels.reshape(chips, 2, own)
    my_labels = jnp.where(core == 0, by_core[:, 0], by_core[:, 1]).reshape(1, samples)
    local = my_labels - chip * (2 * class_rows)
    inside = (local >= 0) & (local < 2 * class_rows)
    turned_ids = jnp.where(core == 0, local, (local + class_rows) % (2 * class_rows))
    ids = jnp.where(inside, turned_ids, -1)

    low, goal = center_directions(ids, own, centers, other_centers)
    early = 6
    exps, pull, report, target_cos = exponentials(ids, x, goal, low, chips, early)
    report = to_chips(report)
    pull = pulled(exps, low, pull, early)
    parcel, scaled, patch, report = settled(ids, target_cos, report, pull, goal, x)
    parcel = to_chips(parcel.reshape(chips, own, depth))

    other_push = pushed(ids, patch, scaled, exps, 1)
    other_push = swapped(other_push)
    grad_centers = pushed(ids, patch, scaled, exps, 0, centers, other_push)

    own_float = embedded.astype(f32)
    inv_emb = inverse_norm(own_float, 1)
    emb_dir = own_float * inv_emb
    grad_dir = jnp.sum(parcel.astype(f32), axis=0)
    grad_emb = (
        (grad_dir - emb_dir * jnp.sum(grad_dir * emb_dir, axis=1, keepdims=True)) * inv_emb
    ).astype(bf16)
    grads = from_chips(grad_emb).reshape(samples, depth)

    fcols = wide // (2 * chips)
    columns, their_columns = x[:, depth : depth + 128], x[:, depth + 128 :]
    turned = (((0,), (0,)), ((), ()))
    theirs_fc = lax.dot_general(their_columns, grads, turned, preferred_element_type=f32)[:fcols]
    theirs_fc = swapped(theirs_fc)
    own_fc = lax.dot_general(columns, grads, turned, preferred_element_type=f32)[:fcols]
    own_fc, theirs_fc = lax.optimization_barrier((own_fc, theirs_fc))
    grad_fc = own_fc + theirs_fc
    own_sums = lax.dynamic_slice_in_dim(report[0], chip * own, own)
    own_logits = lax.dynamic_slice_in_dim(report[0], samples + chip * own % 128, own)
    loss = jnp.log(own_sums) - own_logits
    return (loss, grad_centers, grad_fc)


def solution(mesh):
    torus = Mesh(mesh.devices.reshape(4, 4, 4, 2), CLS)
    placed = (P(CLS, None), P(), P(CLS, None), P())
    return jax.shard_map(
        step,
        mesh=torus,
        in_specs=placed,
        out_specs=(P(CLS), P(CLS, None), P(CLS, None)),
        check_vma=False,
    )
```

```python
import functools
import math

import jax
import jax.numpy as jnp
from jax import lax
from jax.experimental import pallas as pl
from jax.experimental.pallas import tpu as pltpu
from jax.sharding import Mesh
from jax.sharding import PartitionSpec as P


CLS = ("cls_0", "cls_1", "cls_2", "cls_3")
CHIP = ("cls_0", "cls_1", "cls_2")
CORE = "cls_3"

logit_scale = 64.0
cos_margin = math.cos(0.5)
sin_margin = math.sin(0.5)
epsilon = 1e-06

f32 = jnp.float32
bf16 = jnp.bfloat16


def in_hbm(x):
    return pltpu.with_memory_space_constraint(x, pltpu.HBM)


def swapped(x):
    return lax.ppermute(x, CORE, [(0, 1), (1, 0)])


def to_chips(x):
    return lax.all_to_all(x, CHIP, split_axis=0, concat_axis=0, tiled=True)


def from_chips(x):
    copies = jnp.broadcast_to(x, (lax.axis_size(CHIP), *x.shape))
    return lax.all_to_all(copies, CHIP, split_axis=0, concat_axis=0, tiled=True)


def inverse_norm(values, axis):
    return lax.rsqrt(jnp.sum(values * values, axis=axis, keepdims=True) + epsilon)


def margin(target_cos):
    target_sine = jnp.sqrt(1.0 - target_cos * target_cos)
    margined = target_cos * cos_margin - target_sine * sin_margin
    slope = cos_margin + sin_margin * target_cos / target_sine
    return margined, slope


ANY = pl.BlockSpec(memory_space=pl.ANY)
VMEM = pl.BlockSpec(memory_space=pltpu.VMEM)
SMEM = pl.BlockSpec(memory_space=pltpu.SMEM)


def embed_kernel(cuts, core_ref, f_ref, w_ref, out_ref, parcel_ref, weight, sems):
    copies = [
        pltpu.make_async_copy(w_ref.at[pl.ds(a, b - a)], weight.at[pl.ds(a, b - a)], sems.at[k])
        for k, (a, b) in enumerate(zip(cuts, cuts[1:]))
    ]
    for copy in copies:
        copy.start()
    chips = parcel_ref.shape[0]
    own, wide = f_ref.shape
    depth = out_ref.shape[1]
    fcols = wide // (2 * chips)
    lower = core_ref[0] == 0
    pad = jnp.zeros((own, 128 - fcols), bf16)
    for chip in range(chips):
        at = 2 * chip * fcols
        first = jnp.concatenate([f_ref[:, at : at + fcols], pad], axis=1)
        second = jnp.concatenate([f_ref[:, at + fcols : at + 2 * fcols], pad], axis=1)
        parcel_ref[chip, :, depth : depth + 128] = jnp.where(lower, first, second)
        parcel_ref[chip, :, depth + 128 :] = jnp.where(lower, second, first)
    total = None
    for copy, a, b in zip(copies, cuts, cuts[1:]):
        copy.wait()
        product = jnp.dot(f_ref[:, a:b], weight[a:b, :], preferred_element_type=f32)
        total = product if total is None else total + product
    rows = total.astype(bf16)
    out_ref[...] = rows
    rows = rows.astype(f32)
    low = (rows * inverse_norm(rows, 1)).astype(bf16)
    for chip in range(chips):
        parcel_ref[chip, :, :depth] = low


def embedded_rows(core, features, weight, chips, cuts):
    own, wide = features.shape
    depth = weight.shape[1]
    return pl.pallas_call(
        functools.partial(embed_kernel, cuts),
        in_specs=[SMEM, VMEM, ANY],
        out_specs=[VMEM, VMEM],
        out_shape=[
            jax.ShapeDtypeStruct((own, depth), bf16),
            jax.ShapeDtypeStruct((chips, own, depth + 256), bf16),
        ],
        scratch_shapes=[pltpu.VMEM((wide, depth), bf16), pltpu.SemaphoreType.DMA((len(cuts) - 1,))],
        cost_estimate=pl.CostEstimate(
            flops=2 * own * wide * depth, bytes_accessed=2 * wide * depth, transcendentals=0
        ),
        name="embed",
    )(core, features, weight)


def centers_kernel(batch, rows, ids_ref, busy_ref, own_ref, other_ref, low_ref, goal_ref, centers, found, in_sems,
                   out_sems):
    count, depth = own_ref.shape
    steps = 2 * count // rows

    def arrival(i):
        source = own_ref if i * rows < count else other_ref
        return pltpu.make_async_copy(
            source.at[pl.ds(i * rows % count, rows)], centers.at[pl.ds(i * rows, rows)], in_sems.at[i]
        )

    def departure(i):
        span = pl.ds(i * rows, rows)
        return pltpu.make_async_copy(centers.at[span], low_ref.at[span], out_sems.at[i])

    for i in range(steps):
        arrival(i).start()
    found[...] = jnp.zeros_like(found)
    for i in range(steps):
        arrival(i).wait()
        block = centers[i * rows : (i + 1) * rows, :].astype(f32)
        centers[i * rows : (i + 1) * rows, :] = (block * inverse_norm(block, 1)).astype(bf16)
        if i > 0:
            departure(i - 1).start()
    spot = lax.broadcasted_iota(jnp.int32, (16, depth), 0)

    def group(g, carry):
        @pl.when(busy_ref[g] >= 0)
        def _():
            def sample(b, carry):
                at = g * batch + b
                row = ids_ref[0, at]

                @pl.when(row >= 0)
                def _():
                    near = centers[pl.ds(pl.multiple_of(row // 16 * 16, 16), 16), :].astype(f32)
                    found[pl.ds(at, 1), :] = jnp.sum(jnp.where(spot == row % 16, near, 0.0), axis=0, keepdims=True)

                return carry

            lax.fori_loop(0, batch, sample, 0)

        return carry

    lax.fori_loop(0, busy_ref.shape[0], group, 0)
    departure(steps - 1).start()
    goal_ref[...] = found[...].astype(bf16)
    for i in range(steps):
        departure(i).wait()


def center_directions(ids, batch, own, other, rows=1024):
    count, depth = own.shape
    samples = ids.shape[1]
    steps = 2 * count // rows
    busy = jnp.max(ids.reshape(samples // batch, batch), axis=1)
    return pl.pallas_call(
        functools.partial(centers_kernel, batch, rows),
        in_specs=[SMEM, SMEM, ANY, ANY],
        out_specs=[ANY, VMEM],
        out_shape=[
            jax.ShapeDtypeStruct((2 * count, depth), bf16),
            jax.ShapeDtypeStruct((samples, depth), bf16),
        ],
        scratch_shapes=[
            pltpu.VMEM((2 * count, depth), bf16),
            pltpu.VMEM((samples, depth), f32),
            pltpu.SemaphoreType.DMA((steps,)),
            pltpu.SemaphoreType.DMA((steps,)),
        ],
        cost_estimate=pl.CostEstimate(
            flops=2 * count * depth * samples, bytes_accessed=8 * count * depth, transcendentals=0
        ),
        name="targets",
    )(ids, busy, own, other)


def row_of(values):
    part = values[:, :128]
    for k in range(1, values.shape[1] // 128):
        part = part + values[:, k * 128 : (k + 1) * 128]
    return jnp.sum(part.T, axis=0, keepdims=True)


def exp_kernel(early, lanes, ids_ref, x_ref, goal_ref, low_ref, exp_ref, pull_ref,
               report_ref, cos_ref, wide_ids, scaled, row_sum, total):
    i = pl.program_id(0)
    rows = low_ref.shape[0]
    samples = x_ref.shape[0]
    sub = samples // lanes

    @pl.when(i == 0)
    def _():
        wide_ids[...] = jnp.broadcast_to(ids_ref[...], (128, samples)).T
        scaled[...] = (x_ref[...].astype(f32) * logit_scale).astype(bf16)
        row_sum[...] = jnp.zeros_like(row_sum)
        total[...] = jnp.zeros_like(total)

    def chunk(with_pull):
        columns = lax.broadcasted_iota(jnp.int32, (sub, 128), 1)

        def products(m):
            return lax.dot_general(
                scaled[m * sub : (m + 1) * sub, :],
                low_ref[...],
                (((1,), (1,)), ((), ())),
                preferred_element_type=f32,
            )

        logits = products(0)
        for m in range(lanes):
            later = products(m + 1) if m + 1 < lanes else None
            span = slice(m * sub, (m + 1) * sub)
            ids = wide_ids[span, :] - i * rows
            part = None
            for t in range(rows // 128):
                weight = jnp.exp(logits[:, t * 128 : (t + 1) * 128])
                weight = jnp.where(columns + t * 128 == ids, 0.0, weight)
                part = weight if part is None else part + weight
                exp_ref[span, t * 128 : (t + 1) * 128] = weight.astype(bf16)
            row_sum[span, :] += part
            if with_pull:
                total[span, :] += jnp.dot(exp_ref[span, :], low_ref[...], preferred_element_type=f32)
            logits = later

    @pl.when(i < early)
    def _():
        chunk(True)

    @pl.when(i >= early)
    def _():
        chunk(False)

    @pl.when(i == early)
    def _():
        pull_ref[...] = total[...]

    @pl.when(i == pl.num_programs(0) - 1)
    def _():
        target_cos = row_of(goal_ref[...].astype(f32) * scaled[...].astype(f32)) * (1.0 / logit_scale)
        cos_ref[...] = target_cos
        margined, _ = margin(target_cos)
        is_here = ids_ref[...] >= 0
        logit = jnp.where(is_here, logit_scale * margined, 0.0)
        sums = row_of(row_sum[...]) + jnp.where(is_here, jnp.exp(logit_scale * margined), 0.0)
        chips = report_ref.shape[0]
        own = samples // chips
        lane = lax.broadcasted_iota(jnp.int32, (1, 128), 1)
        for chip in range(chips):
            k = chip * own // 128
            theirs = (lane + k * 128) // own == chip
            report_ref[chip, :, :samples] = sums
            report_ref[chip, :, samples:] = jnp.where(theirs, logit[:, k * 128 : (k + 1) * 128], 0.0)


def exponentials(ids, x, goal, low, chips, early, rows=1024, lanes=2):
    samples = x.shape[0]
    count, depth = low.shape
    fixed = lambda i: (0, 0)
    return pl.pallas_call(
        functools.partial(exp_kernel, early, lanes),
        grid=(count // rows,),
        in_specs=[
            pl.BlockSpec((1, samples), fixed),
            pl.BlockSpec((samples, depth), fixed),
            pl.BlockSpec((samples, depth), fixed),
            pl.BlockSpec((rows, depth), lambda i: (i, 0)),
        ],
        out_specs=[
            pl.BlockSpec((samples, rows), lambda i: (0, i)),
            pl.BlockSpec((samples, depth), fixed),
            pl.BlockSpec((chips, 1, samples + 128), lambda i: (0, 0, 0)),
            pl.BlockSpec((1, samples), fixed),
        ],
        out_shape=[
            pltpu.HBM((samples, count), bf16),
            pltpu.HBM((samples, depth), f32),
            jax.ShapeDtypeStruct((chips, 1, samples + 128), f32),
            jax.ShapeDtypeStruct((1, samples), f32),
        ],
        scratch_shapes=[
            pltpu.VMEM((samples, 128), jnp.int32),
            pltpu.VMEM((samples, depth), bf16),
            pltpu.VMEM((samples, 128), f32),
            pltpu.VMEM((samples, depth), f32),
        ],
        compiler_params=pltpu.CompilerParams(vmem_limit_bytes=40 * 1024 * 1024),
        cost_estimate=pl.CostEstimate(
            flops=2 * count * depth * samples,
            bytes_accessed=4 * count * depth,
            transcendentals=count * samples,
        ),
        name="exponentials",
    )(ids, x, in_hbm(goal), in_hbm(low))


def pull_kernel(early, rows, exp_ref, low_ref, start_ref, out_ref, exps, lows, exp_sems, low_sems, start_sem):
    steps = low_ref.shape[0] // rows - early
    start = pltpu.make_async_copy(start_ref, out_ref, start_sem)

    def fetch(i, slot):
        return (
            pltpu.make_async_copy(
                exp_ref.at[:, pl.ds((early + i) * rows, rows)], exps.at[slot], exp_sems.at[slot]
            ),
            pltpu.make_async_copy(low_ref.at[pl.ds((early + i) * rows, rows)], lows.at[slot], low_sems.at[slot]),
        )

    for i in range(steps):
        for copy in fetch(i, i):
            copy.start()
        if i == 0:
            start.start()
    for i in range(steps):
        for copy in fetch(i, i):
            copy.wait()
        if i == 0:
            start.wait()
        out_ref[...] += jnp.dot(exps[i], lows[i], preferred_element_type=f32)


def pulled(exps, low, start, early, rows=1024):
    samples = exps.shape[0]
    count, depth = low.shape
    steps = count // rows - early
    return pl.pallas_call(
        functools.partial(pull_kernel, early, rows),
        in_specs=[ANY, ANY, ANY],
        out_specs=VMEM,
        out_shape=jax.ShapeDtypeStruct((samples, depth), f32),
        scratch_shapes=[
            pltpu.VMEM((steps, samples, rows), bf16),
            pltpu.VMEM((steps, rows, depth), bf16),
            pltpu.SemaphoreType.DMA((steps,)),
            pltpu.SemaphoreType.DMA((steps,)),
            pltpu.SemaphoreType.DMA,
        ],
        cost_estimate=pl.CostEstimate(
            flops=2 * steps * rows * depth * samples,
            bytes_accessed=2 * steps * rows * (depth + samples),
            transcendentals=0,
        ),
        name="pull",
    )(exps, low, start)


def settle_kernel(ids_ref, cos_ref, report_ref, pull_ref, goal_ref, emb_ref, parcel_ref, scaled_ref,
                  patch_ref, sums_ref, wide_scale, wide_target):
    i = pl.program_id(0)
    rows, depth = goal_ref.shape
    samples = ids_ref.shape[1]

    @pl.when(i == 0)
    def _():
        report = jnp.sum(report_ref[...], axis=0)
        sums_ref[...] = report
        sums = report[:, :samples]
        margined, slope = margin(cos_ref[...])
        patch = slope * (jnp.exp(logit_scale * margined) - sums)
        patch_ref[...] = patch
        scale = logit_scale / sums
        at_target = jnp.where(ids_ref[...] >= 0, scale * patch, 0.0)
        wide_scale[...] = jnp.broadcast_to(scale, (128, samples)).T
        wide_target[...] = jnp.broadcast_to(at_target, (128, samples)).T

    span = pl.ds(pl.multiple_of(i * rows, rows), rows)
    scale = jnp.concatenate([wide_scale[span, :]] * (depth // 128), axis=1)
    at_target = jnp.concatenate([wide_target[span, :]] * (depth // 128), axis=1)
    parcel_ref[...] = (pull_ref[...] * scale + at_target * goal_ref[...].astype(f32)).astype(bf16)
    scaled_ref[...] = (emb_ref[...].astype(f32) * scale).astype(bf16)


def settled(ids, target_cos, report, pull, goal, emb, rows=512):
    samples, depth = goal.shape
    fixed = lambda i: (0, 0)
    step = lambda i: (i, 0)
    row = pl.BlockSpec((1, samples), fixed)
    return pl.pallas_call(
        settle_kernel,
        grid=(samples // rows,),
        in_specs=[row, row, pl.BlockSpec(report.shape, lambda i: (0, 0, 0))]
        + [pl.BlockSpec((rows, depth), step)] * 3,
        out_specs=[
            pl.BlockSpec((rows, depth), step),
            pl.BlockSpec((rows, depth), step),
            row,
            pl.BlockSpec((1, report.shape[2]), fixed),
        ],
        out_shape=[
            pltpu.HBM((samples, depth), bf16),
            pltpu.HBM((samples, depth), bf16),
            pltpu.HBM((1, samples), f32),
            pltpu.HBM((1, report.shape[2]), f32),
        ],
        scratch_shapes=[pltpu.VMEM((samples, 128), f32), pltpu.VMEM((samples, 128), f32)],
        compiler_params=pltpu.CompilerParams(vmem_limit_bytes=24 * 1024 * 1024),
        cost_estimate=pl.CostEstimate(
            flops=8 * samples * depth, bytes_accessed=14 * samples * depth, transcendentals=0
        ),
        name="settle",
    )(ids, target_cos, report, in_hbm(pull), goal, emb)


def push_kernel(base, final, ids_ref, patch_ref, emb_ref, exp_ref, *refs):
    i = pl.program_id(0)
    samples, rows = exp_ref.shape
    if final:
        c_ref, other_ref, out_ref, wide_ids, wide_patch = refs
    else:
        out_ref, wide_ids, wide_patch = refs

    @pl.when(i == 0)
    def _():
        wide_ids[...] = jnp.broadcast_to(ids_ref[...], (128, samples)).T
        wide_patch[...] = jnp.broadcast_to(patch_ref[...], (128, samples)).T

    ids = jnp.concatenate([wide_ids[...] - (base + i) * rows] * (rows // 128), axis=1)
    patch = jnp.concatenate([wide_patch[...]] * (rows // 128), axis=1)
    hit = lax.broadcasted_iota(jnp.int32, exp_ref.shape, 1) == ids
    weight = jnp.where(hit, patch, exp_ref[...].astype(f32)).astype(bf16)
    push = lax.dot_general(weight, emb_ref[...], (((0,), (0,)), ((), ())), preferred_element_type=f32)
    if final:
        push = push + other_ref[...].astype(f32)
        block = c_ref[...].astype(f32)
        inv = inverse_norm(block, 1)
        unit = block * inv
        push = (push - unit * jnp.sum(push * unit, axis=1, keepdims=True)) * inv
    out_ref[...] = push.astype(bf16)


def pushed(ids, patch, emb, exps, half, centers=None, other=None, rows=1024):
    samples, depth = emb.shape
    count = exps.shape[1] // 2
    base = half * (count // rows)
    final = centers is not None
    fixed = lambda i: (0, 0)
    step = lambda i: (i, 0)
    extra = (centers, other) if final else ()
    return pl.pallas_call(
        functools.partial(push_kernel, base, final),
        grid=(count // rows,),
        in_specs=[
            pl.BlockSpec((1, samples), fixed),
            pl.BlockSpec((1, samples), fixed),
            pl.BlockSpec((samples, depth), fixed),
            pl.BlockSpec((samples, rows), lambda i: (0, base + i)),
        ]
        + [pl.BlockSpec((rows, depth), step)] * len(extra),
        out_specs=pl.BlockSpec((rows, depth), step),
        out_shape=jax.ShapeDtypeStruct((count, depth), bf16),
        scratch_shapes=[pltpu.VMEM((samples, 128), jnp.int32), pltpu.VMEM((samples, 128), f32)],
        cost_estimate=pl.CostEstimate(
            flops=2 * count * depth * samples, bytes_accessed=2 * count * samples, transcendentals=0
        ),
    )(ids, patch, emb, exps, *extra)


def step(features, fc_weight, centers, labels):
    own, wide = features.shape
    class_rows, depth = centers.shape
    chips = lax.axis_size(CHIP)
    chip = lax.axis_index(CHIP)
    core = lax.axis_index(CORE)
    samples = chips * own

    other_centers = swapped(centers)
    cuts = tuple(range(0, wide, 1792)) + (wide,)
    embedded, parcel = embedded_rows(core.reshape(1), features, fc_weight, chips, cuts)
    x = to_chips(parcel).reshape(samples, depth + 256)

    by_core = labels.reshape(chips, 2, own)
    my_labels = jnp.where(core == 0, by_core[:, 0], by_core[:, 1]).reshape(1, samples)
    local = my_labels - chip * (2 * class_rows)
    inside = (local >= 0) & (local < 2 * class_rows)
    turned_ids = jnp.where(core == 0, local, (local + class_rows) % (2 * class_rows))
    ids = jnp.where(inside, turned_ids, -1)

    low, goal = center_directions(ids, own, centers, other_centers)
    early = 6
    exps, pull, report, target_cos = exponentials(ids, x, goal, low, chips, early)
    report = to_chips(report)
    pull = pulled(exps, low, pull, early)
    parcel, scaled, patch, report = settled(ids, target_cos, report, pull, goal, x)
    parcel = to_chips(parcel.reshape(chips, own, depth))

    other_push = pushed(ids, patch, scaled, exps, 1)
    other_push = swapped(other_push)
    grad_centers = pushed(ids, patch, scaled, exps, 0, centers, other_push)

    own_float = embedded.astype(f32)
    inv_emb = inverse_norm(own_float, 1)
    emb_dir = own_float * inv_emb
    grad_dir = jnp.sum(parcel.astype(f32), axis=0)
    grad_emb = (
        (grad_dir - emb_dir * jnp.sum(grad_dir * emb_dir, axis=1, keepdims=True)) * inv_emb
    ).astype(bf16)
    grads = from_chips(grad_emb).reshape(samples, depth)

    fcols = wide // (2 * chips)
    columns, their_columns = x[:, depth : depth + 128], x[:, depth + 128 :]
    turned = (((0,), (0,)), ((), ()))
    theirs_fc = lax.dot_general(their_columns, grads, turned, preferred_element_type=f32)[:fcols]
    theirs_fc = swapped(theirs_fc)
    own_fc = lax.dot_general(columns, grads, turned, preferred_element_type=f32)[:fcols]
    own_fc, theirs_fc = lax.optimization_barrier((own_fc, theirs_fc))
    grad_fc = own_fc + theirs_fc
    own_sums = lax.dynamic_slice_in_dim(report[0], chip * own, own)
    own_logits = lax.dynamic_slice_in_dim(report[0], samples + chip * own % 128, own)
    loss = jnp.log(own_sums) - own_logits
    return (loss, grad_centers, grad_fc)


def solution(mesh):
    torus = Mesh(mesh.devices.reshape(4, 4, 4, 2), CLS)
    placed = (P(CLS, None), P(), P(CLS, None), P())
    return jax.shard_map(
        step,
        mesh=torus,
        in_specs=placed,
        out_specs=(P(CLS), P(CLS, None), P(CLS, None)),
        check_vma=False,
    )
```

```python
import functools
import math

import jax
import jax.numpy as jnp
from jax import lax
from jax.experimental import pallas as pl
from jax.experimental.pallas import tpu as pltpu
from jax.sharding import Mesh
from jax.sharding import PartitionSpec as P


CLS = ("cls_0", "cls_1", "cls_2", "cls_3")
CHIP = ("cls_0", "cls_1", "cls_2")
CORE = "cls_3"

logit_scale = 64.0
cos_margin = math.cos(0.5)
sin_margin = math.sin(0.5)
epsilon = 1e-06

f32 = jnp.float32
bf16 = jnp.bfloat16


def in_hbm(x):
    return pltpu.with_memory_space_constraint(x, pltpu.HBM)


def swapped(x):
    return lax.ppermute(x, CORE, [(0, 1), (1, 0)])


def to_chips(x):
    return lax.all_to_all(x, CHIP, split_axis=0, concat_axis=0, tiled=True)


def inverse_norm(values, axis):
    return lax.rsqrt(jnp.sum(values * values, axis=axis, keepdims=True) + epsilon)


def margin(target_cos):
    target_sine = jnp.sqrt(1.0 - target_cos * target_cos)
    margined = target_cos * cos_margin - target_sine * sin_margin
    slope = cos_margin + sin_margin * target_cos / target_sine
    return margined, slope


ANY = pl.BlockSpec(memory_space=pl.ANY)
VMEM = pl.BlockSpec(memory_space=pltpu.VMEM)
SMEM = pl.BlockSpec(memory_space=pltpu.SMEM)


def embed_kernel(cuts, core_ref, f_ref, w_ref, out_ref, parcel_ref, weight, sems):
    copies = [
        pltpu.make_async_copy(w_ref.at[pl.ds(a, b - a)], weight.at[pl.ds(a, b - a)], sems.at[k])
        for k, (a, b) in enumerate(zip(cuts, cuts[1:]))
    ]
    for copy in copies:
        copy.start()
    chips = parcel_ref.shape[0]
    own, wide = f_ref.shape
    depth = out_ref.shape[1]
    fcols = wide // (2 * chips)
    lower = core_ref[0] == 0
    pad = jnp.zeros((own, 128 - fcols), bf16)
    for chip in range(chips):
        at = 2 * chip * fcols
        first = jnp.concatenate([f_ref[:, at : at + fcols], pad], axis=1)
        second = jnp.concatenate([f_ref[:, at + fcols : at + 2 * fcols], pad], axis=1)
        parcel_ref[chip, :, depth : depth + 128] = jnp.where(lower, first, second)
        parcel_ref[chip, :, depth + 128 :] = jnp.where(lower, second, first)
    total = None
    for copy, a, b in zip(copies, cuts, cuts[1:]):
        copy.wait()
        product = jnp.dot(f_ref[:, a:b], weight[a:b, :], preferred_element_type=f32)
        total = product if total is None else total + product
    rows = total.astype(bf16)
    out_ref[...] = rows
    rows = rows.astype(f32)
    low = (rows * inverse_norm(rows, 1)).astype(bf16)
    for chip in range(chips):
        parcel_ref[chip, :, :depth] = low


def embedded_rows(core, features, weight, chips, cuts):
    own, wide = features.shape
    depth = weight.shape[1]
    return pl.pallas_call(
        functools.partial(embed_kernel, cuts),
        in_specs=[SMEM, VMEM, ANY],
        out_specs=[VMEM, VMEM],
        out_shape=[
            jax.ShapeDtypeStruct((own, depth), bf16),
            jax.ShapeDtypeStruct((chips, own, depth + 256), bf16),
        ],
        scratch_shapes=[pltpu.VMEM((wide, depth), bf16), pltpu.SemaphoreType.DMA((len(cuts) - 1,))],
        cost_estimate=pl.CostEstimate(
            flops=2 * own * wide * depth, bytes_accessed=2 * wide * depth, transcendentals=0
        ),
        name="embed",
    )(core, features, weight)


def centers_kernel(batch, rows, ids_ref, busy_ref, own_ref, other_ref, low_ref, goal_ref, centers, found, in_sems,
                   out_sems):
    count, depth = own_ref.shape
    steps = 2 * count // rows

    def arrival(i):
        source = own_ref if i * rows < count else other_ref
        return pltpu.make_async_copy(
            source.at[pl.ds(i * rows % count, rows)], centers.at[pl.ds(i * rows, rows)], in_sems.at[i]
        )

    def departure(i):
        span = pl.ds(i * rows, rows)
        return pltpu.make_async_copy(centers.at[span], low_ref.at[span], out_sems.at[i])

    for i in range(steps):
        arrival(i).start()
    found[...] = jnp.zeros_like(found)
    for i in range(steps):
        arrival(i).wait()
        block = centers[i * rows : (i + 1) * rows, :].astype(f32)
        centers[i * rows : (i + 1) * rows, :] = (block * inverse_norm(block, 1)).astype(bf16)
        if i > 0:
            departure(i - 1).start()
    spot = lax.broadcasted_iota(jnp.int32, (16, depth), 0)

    def group(g, carry):
        @pl.when(busy_ref[g] >= 0)
        def _():
            def sample(b, carry):
                at = g * batch + b
                row = ids_ref[0, at]

                @pl.when(row >= 0)
                def _():
                    near = centers[pl.ds(pl.multiple_of(row // 16 * 16, 16), 16), :].astype(f32)
                    found[pl.ds(at, 1), :] = jnp.sum(jnp.where(spot == row % 16, near, 0.0), axis=0, keepdims=True)

                return carry

            lax.fori_loop(0, batch, sample, 0)

        return carry

    lax.fori_loop(0, busy_ref.shape[0], group, 0)
    departure(steps - 1).start()
    goal_ref[...] = found[...].astype(bf16)
    for i in range(steps):
        departure(i).wait()


def center_directions(ids, batch, own, other, rows=1024):
    count, depth = own.shape
    samples = ids.shape[1]
    steps = 2 * count // rows
    busy = jnp.max(ids.reshape(samples // batch, batch), axis=1)
    return pl.pallas_call(
        functools.partial(centers_kernel, batch, rows),
        in_specs=[SMEM, SMEM, ANY, ANY],
        out_specs=[ANY, VMEM],
        out_shape=[
            jax.ShapeDtypeStruct((2 * count, depth), bf16),
            jax.ShapeDtypeStruct((samples, depth), bf16),
        ],
        scratch_shapes=[
            pltpu.VMEM((2 * count, depth), bf16),
            pltpu.VMEM((samples, depth), f32),
            pltpu.SemaphoreType.DMA((steps,)),
            pltpu.SemaphoreType.DMA((steps,)),
        ],
        cost_estimate=pl.CostEstimate(
            flops=2 * count * depth * samples, bytes_accessed=8 * count * depth, transcendentals=0
        ),
        name="targets",
    )(ids, busy, own, other)


def row_of(values):
    part = values[:, :128]
    for k in range(1, values.shape[1] // 128):
        part = part + values[:, k * 128 : (k + 1) * 128]
    return jnp.sum(part.T, axis=0, keepdims=True)


def exp_kernel(early, lanes, ids_ref, x_ref, goal_ref, low_ref, exp_ref, pull_ref,
               report_ref, cos_ref, wide_ids, scaled, row_sum, total):
    i = pl.program_id(0)
    rows = low_ref.shape[0]
    samples = x_ref.shape[0]
    sub = samples // lanes

    @pl.when(i == 0)
    def _():
        wide_ids[...] = jnp.broadcast_to(ids_ref[...], (128, samples)).T
        scaled[...] = (x_ref[...].astype(f32) * logit_scale).astype(bf16)
        row_sum[...] = jnp.zeros_like(row_sum)
        total[...] = jnp.zeros_like(total)

    def chunk(with_pull):
        columns = lax.broadcasted_iota(jnp.int32, (sub, 128), 1)

        def products(m):
            return lax.dot_general(
                scaled[m * sub : (m + 1) * sub, :],
                low_ref[...],
                (((1,), (1,)), ((), ())),
                preferred_element_type=f32,
            )

        logits = products(0)
        for m in range(lanes):
            later = products(m + 1) if m + 1 < lanes else None
            span = slice(m * sub, (m + 1) * sub)
            ids = wide_ids[span, :] - i * rows
            part = None
            for t in range(rows // 128):
                weight = jnp.exp(logits[:, t * 128 : (t + 1) * 128])
                weight = jnp.where(columns + t * 128 == ids, 0.0, weight)
                part = weight if part is None else part + weight
                exp_ref[span, t * 128 : (t + 1) * 128] = weight.astype(bf16)
            row_sum[span, :] += part
            if with_pull:
                total[span, :] += jnp.dot(exp_ref[span, :], low_ref[...], preferred_element_type=f32)
            logits = later

    @pl.when(i < early)
    def _():
        chunk(True)

    @pl.when(i >= early)
    def _():
        chunk(False)

    @pl.when(i == early)
    def _():
        pull_ref[...] = total[...]

    @pl.when(i == pl.num_programs(0) - 1)
    def _():
        target_cos = row_of(goal_ref[...].astype(f32) * scaled[...].astype(f32)) * (1.0 / logit_scale)
        cos_ref[...] = target_cos
        margined, _ = margin(target_cos)
        is_here = ids_ref[...] >= 0
        logit = jnp.where(is_here, logit_scale * margined, 0.0)
        sums = row_of(row_sum[...]) + jnp.where(is_here, jnp.exp(logit_scale * margined), 0.0)
        chips = report_ref.shape[0]
        own = samples // chips
        lane = lax.broadcasted_iota(jnp.int32, (1, 128), 1)
        for chip in range(chips):
            k = chip * own // 128
            theirs = (lane + k * 128) // own == chip
            report_ref[chip, :, :samples] = sums
            report_ref[chip, :, samples:] = jnp.where(theirs, logit[:, k * 128 : (k + 1) * 128], 0.0)


def exponentials(ids, x, goal, low, chips, early, rows=1024, lanes=2):
    samples = x.shape[0]
    count, depth = low.shape
    fixed = lambda i: (0, 0)
    return pl.pallas_call(
        functools.partial(exp_kernel, early, lanes),
        grid=(count // rows,),
        in_specs=[
            pl.BlockSpec((1, samples), fixed),
            pl.BlockSpec((samples, depth), fixed),
            pl.BlockSpec((samples, depth), fixed),
            pl.BlockSpec((rows, depth), lambda i: (i, 0)),
        ],
        out_specs=[
            pl.BlockSpec((samples, rows), lambda i: (0, i)),
            pl.BlockSpec((samples, depth), fixed),
            pl.BlockSpec((chips, 1, samples + 128), lambda i: (0, 0, 0)),
            pl.BlockSpec((1, samples), fixed),
        ],
        out_shape=[
            pltpu.HBM((samples, count), bf16),
            pltpu.HBM((samples, depth), f32),
            jax.ShapeDtypeStruct((chips, 1, samples + 128), f32),
            jax.ShapeDtypeStruct((1, samples), f32),
        ],
        scratch_shapes=[
            pltpu.VMEM((samples, 128), jnp.int32),
            pltpu.VMEM((samples, depth), bf16),
            pltpu.VMEM((samples, 128), f32),
            pltpu.VMEM((samples, depth), f32),
        ],
        compiler_params=pltpu.CompilerParams(vmem_limit_bytes=40 * 1024 * 1024),
        cost_estimate=pl.CostEstimate(
            flops=2 * count * depth * samples,
            bytes_accessed=4 * count * depth,
            transcendentals=count * samples,
        ),
        name="exponentials",
    )(ids, x, in_hbm(goal), in_hbm(low))


def pull_kernel(early, rows, exp_ref, low_ref, start_ref, out_ref, exps, lows, exp_sems, low_sems, start_sem):
    steps = low_ref.shape[0] // rows - early
    start = pltpu.make_async_copy(start_ref, out_ref, start_sem)

    def fetch(i, slot):
        return (
            pltpu.make_async_copy(
                exp_ref.at[:, pl.ds((early + i) * rows, rows)], exps.at[slot], exp_sems.at[slot]
            ),
            pltpu.make_async_copy(low_ref.at[pl.ds((early + i) * rows, rows)], lows.at[slot], low_sems.at[slot]),
        )

    for i in range(steps):
        for copy in fetch(i, i):
            copy.start()
        if i == 0:
            start.start()
    for i in range(steps):
        for copy in fetch(i, i):
            copy.wait()
        if i == 0:
            start.wait()
        out_ref[...] += jnp.dot(exps[i], lows[i], preferred_element_type=f32)


def pulled(exps, low, start, early, rows=1024):
    samples = exps.shape[0]
    count, depth = low.shape
    steps = count // rows - early
    return pl.pallas_call(
        functools.partial(pull_kernel, early, rows),
        in_specs=[ANY, ANY, ANY],
        out_specs=VMEM,
        out_shape=jax.ShapeDtypeStruct((samples, depth), f32),
        scratch_shapes=[
            pltpu.VMEM((steps, samples, rows), bf16),
            pltpu.VMEM((steps, rows, depth), bf16),
            pltpu.SemaphoreType.DMA((steps,)),
            pltpu.SemaphoreType.DMA((steps,)),
            pltpu.SemaphoreType.DMA,
        ],
        cost_estimate=pl.CostEstimate(
            flops=2 * steps * rows * depth * samples,
            bytes_accessed=2 * steps * rows * (depth + samples),
            transcendentals=0,
        ),
        name="pull",
    )(exps, low, start)


def settle_kernel(ids_ref, cos_ref, report_ref, pull_ref, goal_ref, emb_ref, parcel_ref, scaled_ref,
                  patch_ref, sums_ref, wide_scale, wide_target):
    i = pl.program_id(0)
    rows, depth = goal_ref.shape
    samples = ids_ref.shape[1]

    @pl.when(i == 0)
    def _():
        report = jnp.sum(report_ref[...], axis=0)
        sums_ref[...] = report
        sums = report[:, :samples]
        margined, slope = margin(cos_ref[...])
        patch = slope * (jnp.exp(logit_scale * margined) - sums)
        patch_ref[...] = patch
        scale = logit_scale / sums
        at_target = jnp.where(ids_ref[...] >= 0, scale * patch, 0.0)
        wide_scale[...] = jnp.broadcast_to(scale, (128, samples)).T
        wide_target[...] = jnp.broadcast_to(at_target, (128, samples)).T

    span = pl.ds(pl.multiple_of(i * rows, rows), rows)
    scale = jnp.concatenate([wide_scale[span, :]] * (depth // 128), axis=1)
    at_target = jnp.concatenate([wide_target[span, :]] * (depth // 128), axis=1)
    parcel_ref[...] = (pull_ref[...] * scale + at_target * goal_ref[...].astype(f32)).astype(bf16)
    scaled_ref[...] = (emb_ref[...].astype(f32) * scale).astype(bf16)


def settled(ids, target_cos, report, pull, goal, emb, rows=512):
    samples, depth = goal.shape
    fixed = lambda i: (0, 0)
    step = lambda i: (i, 0)
    row = pl.BlockSpec((1, samples), fixed)
    return pl.pallas_call(
        settle_kernel,
        grid=(samples // rows,),
        in_specs=[row, row, pl.BlockSpec(report.shape, lambda i: (0, 0, 0))]
        + [pl.BlockSpec((rows, depth), step)] * 3,
        out_specs=[
            pl.BlockSpec((rows, depth), step),
            pl.BlockSpec((rows, depth), step),
            row,
            pl.BlockSpec((1, report.shape[2]), fixed),
        ],
        out_shape=[
            pltpu.HBM((samples, depth), bf16),
            pltpu.HBM((samples, depth), bf16),
            pltpu.HBM((1, samples), f32),
            pltpu.HBM((1, report.shape[2]), f32),
        ],
        scratch_shapes=[pltpu.VMEM((samples, 128), f32), pltpu.VMEM((samples, 128), f32)],
        compiler_params=pltpu.CompilerParams(vmem_limit_bytes=24 * 1024 * 1024),
        cost_estimate=pl.CostEstimate(
            flops=8 * samples * depth, bytes_accessed=14 * samples * depth, transcendentals=0
        ),
        name="settle",
    )(ids, target_cos, report, in_hbm(pull), goal, emb)


def push_kernel(base, final, ids_ref, patch_ref, emb_ref, exp_ref, *refs):
    i = pl.program_id(0)
    samples, rows = exp_ref.shape
    if final:
        c_ref, other_ref, out_ref, wide_ids, wide_patch = refs
    else:
        out_ref, wide_ids, wide_patch = refs

    @pl.when(i == 0)
    def _():
        wide_ids[...] = jnp.broadcast_to(ids_ref[...], (128, samples)).T
        wide_patch[...] = jnp.broadcast_to(patch_ref[...], (128, samples)).T

    ids = jnp.concatenate([wide_ids[...] - (base + i) * rows] * (rows // 128), axis=1)
    patch = jnp.concatenate([wide_patch[...]] * (rows // 128), axis=1)
    hit = lax.broadcasted_iota(jnp.int32, exp_ref.shape, 1) == ids
    weight = jnp.where(hit, patch, exp_ref[...].astype(f32)).astype(bf16)
    push = lax.dot_general(weight, emb_ref[...], (((0,), (0,)), ((), ())), preferred_element_type=f32)
    if final:
        push = push + other_ref[...].astype(f32)
        block = c_ref[...].astype(f32)
        inv = inverse_norm(block, 1)
        unit = block * inv
        push = (push - unit * jnp.sum(push * unit, axis=1, keepdims=True)) * inv
    out_ref[...] = push.astype(bf16)


def pushed(ids, patch, emb, exps, half, centers=None, other=None, rows=1024):
    samples, depth = emb.shape
    count = exps.shape[1] // 2
    base = half * (count // rows)
    final = centers is not None
    fixed = lambda i: (0, 0)
    step = lambda i: (i, 0)
    extra = (centers, other) if final else ()
    return pl.pallas_call(
        functools.partial(push_kernel, base, final),
        grid=(count // rows,),
        in_specs=[
            pl.BlockSpec((1, samples), fixed),
            pl.BlockSpec((1, samples), fixed),
            pl.BlockSpec((samples, depth), fixed),
            pl.BlockSpec((samples, rows), lambda i: (0, base + i)),
        ]
        + [pl.BlockSpec((rows, depth), step)] * len(extra),
        out_specs=pl.BlockSpec((rows, depth), step),
        out_shape=jax.ShapeDtypeStruct((count, depth), bf16),
        scratch_shapes=[pltpu.VMEM((samples, 128), jnp.int32), pltpu.VMEM((samples, 128), f32)],
        cost_estimate=pl.CostEstimate(
            flops=2 * count * depth * samples, bytes_accessed=2 * count * samples, transcendentals=0
        ),
    )(ids, patch, emb, exps, *extra)


def own_kernel(parcel_ref, emb_ref, copies_ref):
    chips = parcel_ref.shape[0]
    total = parcel_ref[0].astype(f32)
    for chip in range(1, chips):
        total = total + parcel_ref[chip].astype(f32)
    emb = emb_ref[...].astype(f32)
    inv = inverse_norm(emb, 1)
    unit = emb * inv
    grad = ((total - unit * jnp.sum(total * unit, axis=1, keepdims=True)) * inv).astype(bf16)
    for chip in range(chips):
        copies_ref[chip] = grad


def own_gradients(parcel, embedded):
    return pl.pallas_call(
        own_kernel,
        in_specs=[VMEM, VMEM],
        out_specs=VMEM,
        out_shape=pltpu.HBM(parcel.shape, bf16),
        compiler_params=pltpu.CompilerParams(vmem_limit_bytes=24 * 1024 * 1024),
        cost_estimate=pl.CostEstimate(
            flops=parcel.size, bytes_accessed=4 * parcel.size, transcendentals=0
        ),
        name="own",
    )(parcel, embedded)


def step(features, fc_weight, centers, labels):
    own, wide = features.shape
    class_rows, depth = centers.shape
    chips = lax.axis_size(CHIP)
    chip = lax.axis_index(CHIP)
    core = lax.axis_index(CORE)
    samples = chips * own

    other_centers = swapped(centers)
    cuts = tuple(range(0, wide, 1792)) + (wide,)
    embedded, parcel = embedded_rows(core.reshape(1), features, fc_weight, chips, cuts)
    x = to_chips(parcel).reshape(samples, depth + 256)

    by_core = labels.reshape(chips, 2, own)
    my_labels = jnp.where(core == 0, by_core[:, 0], by_core[:, 1]).reshape(1, samples)
    local = my_labels - chip * (2 * class_rows)
    inside = (local >= 0) & (local < 2 * class_rows)
    turned_ids = jnp.where(core == 0, local, (local + class_rows) % (2 * class_rows))
    ids = jnp.where(inside, turned_ids, -1)

    low, goal = center_directions(ids, own, centers, other_centers)
    early = 6
    exps, pull, report, target_cos = exponentials(ids, x, goal, low, chips, early)
    report = to_chips(report)
    pull = pulled(exps, low, pull, early)
    parcel, scaled, patch, report = settled(ids, target_cos, report, pull, goal, x)
    parcel = to_chips(parcel.reshape(chips, own, depth))

    other_push = pushed(ids, patch, scaled, exps, 1)
    other_push = swapped(other_push)
    grad_centers = pushed(ids, patch, scaled, exps, 0, centers, other_push)

    copies = own_gradients(parcel, embedded)
    grads = to_chips(copies).reshape(samples, depth)

    fcols = wide // (2 * chips)
    columns, their_columns = x[:, depth : depth + 128], x[:, depth + 128 :]
    turned = (((0,), (0,)), ((), ()))
    theirs_fc = lax.dot_general(their_columns, grads, turned, preferred_element_type=f32)[:fcols]
    theirs_fc = swapped(theirs_fc)
    own_fc = lax.dot_general(columns, grads, turned, preferred_element_type=f32)[:fcols]
    own_fc, theirs_fc = lax.optimization_barrier((own_fc, theirs_fc))
    grad_fc = own_fc + theirs_fc
    own_sums = lax.dynamic_slice_in_dim(report[0], chip * own, own)
    own_logits = lax.dynamic_slice_in_dim(report[0], samples + chip * own % 128, own)
    loss = jnp.log(own_sums) - own_logits
    return (loss, grad_centers, grad_fc)


def solution(mesh):
    torus = Mesh(mesh.devices.reshape(4, 4, 4, 2), CLS)
    placed = (P(CLS, None), P(), P(CLS, None), P())
    return jax.shard_map(
        step,
        mesh=torus,
        in_specs=placed,
        out_specs=(P(CLS), P(CLS, None), P(CLS, None)),
        check_vma=False,
    )
```
